32 devices in a mesh: shard: 32 (over z, y, x, core).
Axes of the slice: x: 2, y: 2, z: 4, core: 2. Of those that a mesh axis runs over, the one named last changes fastest.
Arguments:
- lookup_ids: int32 [65536], P('shard'), may hold values from 0 to 524287, as said below
- grad_rows: float32 [65536, 128], P('shard'), may hold values from -6 to 6
- emb_table: float32 [524288, 128], P('shard'), may hold values from -4 to 4
- row_accum: float32 [524288], P('shard'), may hold values from 0.01 to 1
Outputs:
- new_table: float32 [524288, 128], P('shard')
- new_accum: float32 [524288], P('shard')
- looked_up: float32 [65536, 128], P('shard')
The draws below stay inside these ranges and needn't reach their ends.
Inputs may be any that keep to these rules, and one draw needn't show every extreme that they name: `lookup_ids`: each device's 2048 lookups name exactly 64 rows, repeats counted, in the range of every owner; within an owner's range the row numbers follow a power law, so that a few rows are named very often.
All inputs are finite; a program needn't handle non-finite values.
Results may differ from the reference program's by a relative error of at most 0.00002.
Values sent between devices are 32-bit elements; how exact they have to be, the bound alone decides.
A program may use at most 64 MiB of HBM per device.

```python
import math
import jax
import jax.numpy as jnp
from jax import lax

W = 128
ROWS_DEV = 16384
LOOK_DEV = 2048
ROWS = 524288
LOOKUPS = 65536
N_SHARD = 32


def draw_lookup_ids(key, part):
    key_perm, key_exp, key_row = jax.random.split(key, 3)
    perm_keys = jax.random.split(key_perm, N_SHARD)
    arrange = jax.vmap(lambda k: jax.random.permutation(k, LOOK_DEV))(perm_keys)
    owners = arrange % N_SHARD
    bit_count = ROWS_DEV.bit_length()
    exponent = jax.random.randint(key_exp, (N_SHARD, LOOK_DEV), 0, bit_count + 1)
    upper_limit = jnp.minimum(jnp.left_shift(jnp.ones_like(exponent), exponent), ROWS_DEV)
    local_rows = jax.random.randint(key_row, (N_SHARD, LOOK_DEV), 0, upper_limit)
    return (owners * ROWS_DEV + local_rows).reshape(-1).astype(jnp.int32)


def level_of(own_key, extent, cuts, low, largest):
    gain = 1.0
    for axis_at, parts in cuts:
        heights = jax.random.uniform(jax.random.fold_in(jax.random.fold_in(own_key, 6), axis_at), (parts,), jnp.float32, low / len(cuts), largest / len(cuts))
        gain = gain * jnp.repeat(jnp.exp(heights), extent[axis_at] // parts).reshape((-1,) + (1,) * (len(extent) - 1 - axis_at))
    return gain


def centred(own_key, dims, deviation, reach, shards=(), held_as=jnp.bfloat16):
    entries = deviation * jax.random.normal(own_key, dims, jnp.float32)
    if shards:
        entries = entries * level_of(own_key, dims, shards, -0.22, 0.18)
    return jnp.clip(entries, -reach, reach).astype(held_as)


def setup_inputs(seed: int = 0) -> dict:
    keys = jax.random.split(jax.random.key(seed), 5)
    return {
        "lookup_ids": draw_lookup_ids(jax.random.fold_in(keys[4], 71), 0),
        "grad_rows": centred(keys[1], (LOOKUPS, W), 1.0, 6.0, ((0, 32),), jnp.float32),
        "emb_table": centred(keys[2], (ROWS, W), 0.5, 4.0, ((0, 32),), jnp.float32),
        "row_accum": jnp.clip(jnp.exp(math.log(1.0) - 4.6051702 * jax.random.uniform(keys[3], (ROWS,), jnp.float32) ** level_of(keys[3], (ROWS,), ((0, 32),), -0.2, 0.2)), 0.01, 1.0),
    }


LEARNING_RATE = 0.5
EPSILON = 1e-08

def reference(lookup_ids, grad_rows, emb_table, row_accum):
    total_rows = emb_table.shape[0]
    summed = jax.ops.segment_sum(grad_rows, lookup_ids, num_segments=total_rows)
    new_accum = row_accum + lax.optimization_barrier(jnp.mean(summed * summed, axis=1))
    new_table = emb_table - LEARNING_RATE * summed / (jnp.sqrt(new_accum)[:, None] + EPSILON)
    looked_up = new_table[lookup_ids]
    return (new_table, new_accum, looked_up)
```

```python
import functools

import jax
import jax.numpy as jnp
from jax import lax
from jax.experimental import pallas as pl
from jax.experimental.pallas import tpu as pltpu
from jax.sharding import PartitionSpec as P

LEARNING_RATE = 0.5
EPSILON = 1e-08
LANES = 128
MIB = 1024 * 1024
BATCH = 16
MESH = pl.DeviceIdType.MESH
F32 = jnp.float32
BF16 = jnp.bfloat16


def split3(x):
    hi = x.astype(BF16)
    rest = x - hi.astype(F32)
    mid = rest.astype(BF16)
    low = (rest - mid.astype(F32)).astype(BF16)
    return hi, mid, low


def dot(a, b):
    return jnp.dot(a, b, preferred_element_type=F32)


def column_of(row):
    return jnp.transpose(jnp.broadcast_to(row, (LANES, LANES)))


def one_hot_bf16(mask):
    return jnp.where(mask, 1.0, 0.0).astype(BF16)


def fill(terms, x, width):
    for i, term in enumerate(split3(x)):
        terms[:, i * width : (i + 1) * width] = term


def joined(x, width):
    return x[:, 0:width] + x[:, width : 2 * width] + x[:, 2 * width : 3 * width]


def quarter_at(half, inner):
    return inner * (1 + half) + (1 - inner) * 3 * half


def greet_all(barrier, me, n):
    def greet(step, carry):
        pl.semaphore_signal(
            barrier, inc=1, device_id=(lax.rem(me + step, n),), device_id_type=MESH
        )
        return carry

    lax.fori_loop(1, n, greet, 0)


def step_kernel(
    n, ids_hbm, grads_hbm, accum_hbm, emb_hbm,
    pos_ref, ids_ref, fresh, new_accum_ref, table, back,
    lookups, grads, accum, send_ids, send, recv_ids, recv, sorted_terms, terms, acc, cols, old_rows,
    weights, hi_hot, ids_smem,
    load_sem, smem_sem, ids_out, ids_in, grads_out, grads_in, back_out, back_in,
):
    blocks = lookups.shape[0]
    look = blocks * LANES
    width = grads.shape[1]
    rows_dev = table.shape[0]
    groups = accum.shape[0]
    per_peer = look // n
    per_row = LANES // per_peer
    quarter = n // 4
    eighth = n // 8
    piece = look // 8
    tile = look // 4
    me = lax.axis_index("shard")
    side = me // (n // 2)
    loads = [
        pltpu.make_async_copy(s, d, load_sem.at[i])
        for i, (s, d) in enumerate(
            ((ids_hbm, lookups), (grads_hbm, grads), (accum_hbm, accum), (emb_hbm, table))
        )
    ]
    for load in loads:
        load.start()
    barrier = pltpu.get_barrier_semaphore()
    greet_all(barrier, me, n)

    loads[0].wait()
    peer_iota = lax.broadcasted_iota(jnp.int32, (n, LANES), 0)
    slot_iota = lax.broadcasted_iota(jnp.int32, (LANES, LANES), 0)
    before = one_hot_bf16(slot_iota < lax.broadcasted_iota(jnp.int32, (LANES, LANES), 1))
    shift = lax.rem(me, per_row) * per_peer
    base = jnp.zeros((n, 1), F32)
    low = peer_iota * rows_dev
    owned, ranked, pos = [], [], []
    for b in range(blocks):
        ids = lookups[b : b + 1, :]
        mine = (ids >= low) & (ids < low + rows_dev)
        hot = jnp.where(mine, 1.0, 0.0)
        rank = dot(hot.astype(BF16), before) + base
        rank = jnp.sum(hot * rank, axis=0, keepdims=True).astype(jnp.int32)
        peer = jnp.sum(jnp.where(mine, peer_iota, 0), axis=0, keepdims=True)
        pos.append(peer * per_peer + rank)
        pos_ref[b : b + 1, :] = pos[b]
        base = base + jnp.sum(hot, axis=1, keepdims=True)
        offset = ids - peer * rows_dev
        digits = [offset & 255, (offset >> 8) & 255, offset >> 16]
        owned.append(jnp.concatenate([hot * d.astype(F32) for d in digits], axis=0).astype(BF16))
        ranked.append(one_hot_bf16(slot_iota == rank + shift))
    named = lax.dot_general(
        jnp.concatenate(owned, axis=1),
        jnp.concatenate(ranked, axis=1),
        (((1,), (1,)), ((), ())),
        preferred_element_type=F32,
    ).astype(jnp.int32)
    named = named[0:n] + named[n : 2 * n] * 256 + named[2 * n : 3 * n] * 65536
    for p in range(n):
        send_ids[p] = named[p : p + 1, :]
    loads[1].wait()
    fill(sorted_terms, grads[...], width)
    pl.semaphore_wait(barrier, n - 1)

    def rows_of(ref, p):
        return ref.at[pl.ds(pl.multiple_of(p * per_peer, 8), per_peer), :]

    def ids_copy(p, source):
        return pltpu.make_async_remote_copy(
            src_ref=send_ids.at[p], dst_ref=recv_ids.at[source],
            send_sem=ids_out.at[p], recv_sem=ids_in.at[source],
            device_id=(p,), device_id_type=MESH,
        )

    def grads_copy(p, source):
        return pltpu.make_async_remote_copy(
            src_ref=rows_of(send, p), dst_ref=rows_of(recv, source),
            send_sem=grads_out.at[p], recv_sem=grads_in.at[source],
            device_id=(p,), device_id_type=MESH,
        )

    def back_copy(p, source):
        return pltpu.make_async_remote_copy(
            src_ref=rows_of(fresh, p), dst_ref=rows_of(back, source),
            send_sem=back_out.at[p], recv_sem=back_in.at[source],
            device_id=(p,), device_id_type=MESH,
        )

    def first_peer(i):
        cross = 1 - lax.rem(i // 2, 2)
        half = cross * (1 - side) + (1 - cross) * side
        target = quarter_at(half, 1 - i // 4)
        return target * quarter + lax.rem(lax.rem(me, quarter) // eighth + i, 2) * eighth

    def start_piece(copy, i):
        def start(s, carry):
            p = first_peer(i) + lax.rem(lax.rem(me, eighth) + s, eighth)

            @pl.when(p != me)
            def _():
                copy(p, me).start()

            return carry

        lax.fori_loop(0, eighth, start, 0)

    def arrange(i):
        begin = pl.multiple_of(first_peer(i) * per_peer, piece)
        place = begin + lax.broadcasted_iota(jnp.int32, (piece, LANES), 0)
        pick = jnp.concatenate([one_hot_bf16(place == p) for p in pos], axis=1)
        send[pl.ds(begin, piece), :] = joined(dot(pick, sorted_terms[...]), width)

    def start_ids(step, carry):
        ids_copy(lax.rem(me + step, n), me).start()
        return carry

    arrange(0)
    lax.fori_loop(1, n, start_ids, 0)

    @pl.loop(1, 8)
    def _(i):
        arrange(i)
        start_piece(grads_copy, i - 1)

    recv_ids[pl.ds(me, 1)] = send_ids[pl.ds(me, 1)]

    def ids_arrive(step, carry):
        p = lax.rem(me + step, n)
        ids_copy(p, p).wait_recv()
        return carry

    lax.fori_loop(1, n, ids_arrive, 0)
    start_piece(grads_copy, 7)
    rows_of(recv, me)[...] = rows_of(send, me)[...]
    for b in range(blocks):
        ids_ref[b : b + 1, :] = sum(recv_ids[b * per_row + k] for k in range(per_row))
    to_smem = pltpu.make_async_copy(ids_ref, ids_smem, smem_sem)
    to_smem.start()

    @pl.loop(0, blocks)
    def _(b):
        here = pl.ds(pl.multiple_of(b * LANES, LANES), LANES)
        cols[here, :] = column_of(ids_ref[pl.ds(b, 1), :])

    loads[2].wait()
    acc3 = jnp.concatenate(split3(accum[...]), axis=1)
    terms[:, 3 * width : 4 * width] = jnp.ones((tile, width), BF16)
    to_smem.wait()
    loads[3].wait()

    @pl.loop(0, blocks)
    def _(b):
        start = pl.multiple_of(b * LANES, LANES)
        for i in range(0, LANES, BATCH):
            picks = [jnp.clip(ids_smem[b, i + k], 0, rows_dev - 1) for k in range(BATCH)]
            batch = [table[pl.ds(pick, 1), :] for pick in picks]
            for k in range(BATCH):
                old_rows[pl.ds(start + i + k, 1), :] = batch[k]

    acc[...] = jnp.zeros_like(acc)

    @pl.loop(0, 4)
    def _(i):
        half = (i // 2) * (1 - side) + (1 - i // 2) * side
        source = 2 * half + lax.rem(me // quarter + i, 2)

        def arrive(s, carry):
            p = source * quarter + s

            @pl.when(p != me)
            def _():
                grads_copy(p, p).wait_recv()

            return carry

        lax.fori_loop(0, quarter, arrive, 0)
        fill(terms, recv[pl.ds(pl.multiple_of(source * tile, tile), tile), :], width)
        lines = tile // LANES
        rows = [ids_ref[pl.ds(source * lines + k, 1), :] for k in range(lines)]

        @pl.loop(0, 4)
        def _(t):
            here = pl.ds(pl.multiple_of(t * tile, tile), tile)
            col = cols[here, :]
            same = jnp.concatenate([one_hot_bf16(col == r) for r in rows], axis=1)
            acc[here, :] += dot(same, terms[...])

    lane = lax.broadcasted_iota(jnp.int32, (piece, LANES), 1)
    group_iota = lax.broadcasted_iota(jnp.int32, (piece, groups), 1)

    @pl.loop(0, 8)
    def _(i):
        here = pl.ds(pl.multiple_of(first_peer(i) * per_peer, piece), piece)
        col = cols[here, :]
        out = acc[here, :]
        summed = joined(out, width)
        times = out[:, 3 * width : 3 * width + 1]
        mean = jnp.sum(summed * summed, axis=1, keepdims=True) * (1.0 / width)
        at_lane = (col & (LANES - 1)) == lane
        at_group = one_hot_bf16((col >> 7)[:, 0:1] == group_iota)
        found = joined(dot(at_group, acc3), LANES)
        new_acc = jnp.sum(jnp.where(at_lane, found, 0.0), axis=1, keepdims=True) + mean
        rate = LEARNING_RATE / (jnp.sqrt(new_acc) + EPSILON)
        fresh[here, :] = old_rows[here, :] - summed * rate
        share = jnp.where(at_lane, jnp.broadcast_to(mean / times, (piece, LANES)), 0.0)
        for k, term in enumerate(split3(share)):
            weights[here, k * LANES : (k + 1) * LANES] = term
        hi_hot[here, :] = at_group

        @pl.when(i > 0)
        def _():
            start_piece(back_copy, i - 1)

    added = lax.dot_general(
        hi_hot[...], weights[...], (((0,), (0,)), ((), ())), preferred_element_type=F32
    )
    new_accum_ref[...] = accum[...] + joined(added, LANES)
    start_piece(back_copy, 7)
    rows_of(back, me)[...] = rows_of(fresh, me)[...]

    def back_arrive(step, carry):
        p = lax.rem(me + step, n)
        back_copy(p, p).wait_recv()
        return carry

    lax.fori_loop(1, n, back_arrive, 0)

    def drain(step, carry):
        p = lax.rem(me + step, n)
        ids_copy(p, me).wait_send()
        grads_copy(p, me).wait_send()
        back_copy(p, me).wait_send()
        return carry

    lax.fori_loop(1, n, drain, 0)


def finish_kernel(
    pos_smem, ids_smem, fresh, back, accum, table_in,
    new_table, new_accum, looked_up, table,
    rows, table_sem, accum_sem, rows_sem,
):
    del table_in
    look = fresh.shape[0]
    blocks = look // LANES
    tile = look // 4
    keep = pltpu.make_async_copy(accum, new_accum, accum_sem)
    keep.start()

    @pl.loop(0, blocks)
    def _(b):
        start = pl.multiple_of(b * LANES, LANES)
        for i in range(0, LANES, BATCH):
            batch = [fresh[pl.ds(start + i + k, 1), :] for k in range(BATCH)]
            for k in range(BATCH):
                table[pl.ds(ids_smem[b, i + k], 1), :] = batch[k]

    store = pltpu.make_async_copy(table, new_table, table_sem)
    store.start()

    def out_copy(t):
        here = pl.ds(pl.multiple_of(t * tile, tile), tile)
        return pltpu.make_async_copy(rows.at[here, :], looked_up.at[here, :], rows_sem.at[t])

    @pl.loop(0, 4)
    def _(t):
        @pl.loop(0, tile // LANES)
        def _(j):
            b = t * (tile // LANES) + j
            start = pl.multiple_of(b * LANES, LANES)
            for i in range(0, LANES, BATCH):
                batch = [back[pl.ds(pos_smem[b, i + k], 1), :] for k in range(BATCH)]
                for k in range(BATCH):
                    rows[pl.ds(start + i + k, 1), :] = batch[k]

        @pl.when(t > 0)
        def _():
            out_copy(t - 1).start()

    keep.wait()
    out_copy(3).start()
    for t in range(4):
        out_copy(t).wait()
    store.wait()


def in_hbm(x):
    return pltpu.with_memory_space_constraint(x, pltpu.HBM)


def on_device(lookup_ids, grad_rows, emb_table, row_accum):
    n = lax.axis_size("shard")
    look, width = grad_rows.shape
    rows_dev = emb_table.shape[0]
    blocks = look // LANES
    groups = rows_dev // LANES
    vmem = pl.BlockSpec(memory_space=pltpu.VMEM)
    smem = pl.BlockSpec(memory_space=pltpu.SMEM)
    hbm = pl.BlockSpec(memory_space=pltpu.HBM)
    tile = look // 4
    dma = pltpu.SemaphoreType.DMA

    pos, local_ids, fresh, accum, table, back = pl.pallas_call(
        functools.partial(step_kernel, n),
        out_shape=[
            pltpu.VMEM((blocks, LANES), jnp.int32),
            pltpu.VMEM((blocks, LANES), jnp.int32),
            pltpu.VMEM((look, width), F32),
            pltpu.VMEM((groups, LANES), F32),
            pltpu.VMEM((rows_dev, width), F32),
            pltpu.VMEM((look, width), F32),
        ],
        in_specs=[hbm] * 4,
        out_specs=[vmem] * 6,
        scratch_shapes=[
            pltpu.VMEM((blocks, LANES), jnp.int32),
            pltpu.VMEM((look, width), F32),
            pltpu.VMEM((groups, LANES), F32),
            pltpu.VMEM((n, 1, LANES), jnp.int32),
            pltpu.VMEM((look, width), F32),
            pltpu.VMEM((n, 1, LANES), jnp.int32),
            pltpu.VMEM((look, width), F32),
            pltpu.VMEM((look, 3 * width), BF16),
            pltpu.VMEM((tile, 4 * width), BF16),
            pltpu.VMEM((look, 4 * width), F32),
            pltpu.VMEM((look, LANES), jnp.int32),
            pltpu.VMEM((look, width), F32),
            pltpu.VMEM((look, 3 * LANES), BF16),
            pltpu.VMEM((look, groups), BF16),
            pltpu.SMEM((blocks, LANES), jnp.int32),
            dma((4,)),
            dma(()),
            dma((n,)),
            dma((n,)),
            dma((n,)),
            dma((n,)),
            dma((n,)),
            dma((n,)),
        ],
        compiler_params=pltpu.CompilerParams(
            collective_id=1, has_side_effects=True, vmem_limit_bytes=44 * MIB
        ),
    )(
        in_hbm(lookup_ids.reshape(blocks, LANES)),
        in_hbm(grad_rows),
        in_hbm(row_accum.reshape(groups, LANES)),
        in_hbm(emb_table),
    )

    new_table, new_accum, looked_up, _ = pl.pallas_call(
        finish_kernel,
        out_shape=[
            jax.ShapeDtypeStruct((rows_dev, width), F32),
            jax.ShapeDtypeStruct((groups, LANES), F32),
            jax.ShapeDtypeStruct((look, width), F32),
            pltpu.VMEM((rows_dev, width), F32),
        ],
        in_specs=[smem, smem, vmem, vmem, vmem, vmem],
        out_specs=[hbm, hbm, hbm, vmem],
        input_output_aliases={5: 3},
        scratch_shapes=[pltpu.VMEM((look, width), F32), dma(()), dma(()), dma((4,))],
        compiler_params=pltpu.CompilerParams(vmem_limit_bytes=24 * MIB),
    )(pos, local_ids, fresh, back, accum, table)
    return (new_table, new_accum.reshape(rows_dev), looked_up)


def solution(mesh):
    in_specs = (P("shard"), P("shard", None), P("shard", None), P("shard"))
    out_specs = (P("shard", None), P("shard"), P("shard", None))
    return jax.shard_map(
        on_device, mesh=mesh, in_specs=in_specs, out_specs=out_specs, check_vma=False
    )
```

```python
import functools

import jax
import jax.numpy as jnp
from jax import lax
from jax.experimental import pallas as pl
from jax.experimental.pallas import tpu as pltpu
from jax.sharding import PartitionSpec as P

LEARNING_RATE = 0.5
EPSILON = 1e-08
LANES = 128
MIB = 1024 * 1024
BATCH = 16
MESH = pl.DeviceIdType.MESH


def order_of(*pieces):
    return sum(piece * 8**i for i, piece in enumerate(pieces))


OUT = order_of(6, 7, 0, 1, 2, 3, 4, 5)
IN_INNER = order_of(2, 3, 1, 0)
IN_OUTER = order_of(0, 1, 2, 3)
BACK_INNER = order_of(4, 6, 0, 5, 7, 1, 2, 3)
BACK_OUTER = order_of(2, 3, 4, 6, 5, 7, 0, 1)
F32 = jnp.float32
BF16 = jnp.bfloat16


def split3(x):
    hi = x.astype(BF16)
    rest = x - hi.astype(F32)
    mid = rest.astype(BF16)
    low = (rest - mid.astype(F32)).astype(BF16)
    return hi, mid, low


def dot(a, b):
    return jnp.dot(a, b, preferred_element_type=F32)


def column_of(row):
    return jnp.transpose(jnp.broadcast_to(row, (LANES, LANES)))


def one_hot_bf16(mask):
    return jnp.where(mask, 1.0, 0.0).astype(BF16)


def fill(terms, x, width):
    for i, term in enumerate(split3(x)):
        terms[:, i * width : (i + 1) * width] = term


def joined(x, width):
    return x[:, 0:width] + x[:, width : 2 * width] + x[:, 2 * width : 3 * width]


def quarter_at(half, inner):
    return inner * (1 + half) + (1 - inner) * 3 * half


def greet_all(barrier, me, n):
    def greet(step, carry):
        pl.semaphore_signal(
            barrier, inc=1, device_id=(lax.rem(me + step, n),), device_id_type=MESH
        )
        return carry

    lax.fori_loop(1, n, greet, 0)


def step_kernel(
    n, ids_hbm, grads_hbm, accum_hbm, emb_hbm,
    pos_ref, ids_ref, fresh, new_accum_ref, table, back,
    lookups, grads, accum, send_ids, send, recv_ids, recv, sorted_terms, terms, acc, cols, old_rows,
    weights, hi_hot, ids_smem,
    load_sem, smem_sem, ids_out, ids_in, grads_out, grads_in, back_out, back_in,
):
    blocks = lookups.shape[0]
    look = blocks * LANES
    width = grads.shape[1]
    rows_dev = table.shape[0]
    groups = accum.shape[0]
    per_peer = look // n
    per_row = LANES // per_peer
    quarter = n // 4
    eighth = n // 8
    piece = look // 8
    tile = look // 4
    me = lax.axis_index("shard")
    side = me // (n // 2)
    floor = me // quarter
    inner = lax.rem(floor + side, 2)
    row = lax.rem(me, quarter) // eighth
    loads = [
        pltpu.make_async_copy(s, d, load_sem.at[i])
        for i, (s, d) in enumerate(
            ((ids_hbm, lookups), (grads_hbm, grads), (accum_hbm, accum), (emb_hbm, table))
        )
    ]
    barrier = pltpu.get_barrier_semaphore()
    for load in loads:
        load.start()
    greet_all(barrier, me, n)

    loads[0].wait()
    peer_iota = lax.broadcasted_iota(jnp.int32, (n, LANES), 0)
    slot_iota = lax.broadcasted_iota(jnp.int32, (LANES, LANES), 0)
    before = one_hot_bf16(slot_iota < lax.broadcasted_iota(jnp.int32, (LANES, LANES), 1))
    shift = lax.rem(me, per_row) * per_peer
    base = jnp.zeros((n, 1), F32)
    low = peer_iota * rows_dev
    owned, ranked, pos = [], [], []
    for b in range(blocks):
        ids = lookups[b : b + 1, :]
        mine = (ids >= low) & (ids < low + rows_dev)
        hot = jnp.where(mine, 1.0, 0.0)
        rank = dot(hot.astype(BF16), before) + base
        rank = jnp.sum(hot * rank, axis=0, keepdims=True).astype(jnp.int32)
        peer = jnp.sum(jnp.where(mine, peer_iota, 0), axis=0, keepdims=True)
        pos.append(peer * per_peer + rank)
        pos_ref[b : b + 1, :] = pos[b]
        base = base + jnp.sum(hot, axis=1, keepdims=True)
        offset = ids - peer * rows_dev
        digits = [offset & 255, (offset >> 8) & 255, offset >> 16]
        owned.append(jnp.concatenate([hot * d.astype(F32) for d in digits], axis=0).astype(BF16))
        ranked.append(one_hot_bf16(slot_iota == rank + shift))
    named = lax.dot_general(
        jnp.concatenate(owned, axis=1),
        jnp.concatenate(ranked, axis=1),
        (((1,), (1,)), ((), ())),
        preferred_element_type=F32,
    ).astype(jnp.int32)
    named = named[0:n] + named[n : 2 * n] * 256 + named[2 * n : 3 * n] * 65536
    for p in range(n):
        send_ids[p] = named[p : p + 1, :]
    loads[1].wait()
    fill(sorted_terms, grads[...], width)

    def rows_of(ref, p):
        return ref.at[pl.ds(pl.multiple_of(p * per_peer, 8), per_peer), :]

    def ids_copy(p, source):
        return pltpu.make_async_remote_copy(
            src_ref=send_ids.at[p], dst_ref=recv_ids.at[source],
            send_sem=ids_out.at[p], recv_sem=ids_in.at[source],
            device_id=(p,), device_id_type=MESH,
        )

    def grads_copy(p, source):
        return pltpu.make_async_remote_copy(
            src_ref=rows_of(send, p), dst_ref=rows_of(recv, source),
            send_sem=grads_out.at[p], recv_sem=grads_in.at[source],
            device_id=(p,), device_id_type=MESH,
        )

    def back_copy(p, source):
        return pltpu.make_async_remote_copy(
            src_ref=rows_of(fresh, p), dst_ref=rows_of(back, source),
            send_sem=back_out.at[p], recv_sem=back_in.at[source],
            device_id=(p,), device_id_type=MESH,
        )

    def mine(at_inner, at_outer):
        return inner * at_inner + (1 - inner) * at_outer

    def digit_of(order, i):
        return lax.rem(lax.shift_right_logical(jnp.int32(order), jnp.int32(3 * i)), 8)

    def first_peer(order, i):
        piece_at = digit_of(order, i)
        cross, middle, turn = piece_at // 4, lax.rem(piece_at // 2, 2), lax.rem(piece_at, 2)
        half = cross * (1 - side) + (1 - cross) * side
        return quarter_at(half, middle) * quarter + lax.rem(row + turn, 2) * eighth

    def first_out(i):
        return first_peer(OUT, i)

    def first_back(i):
        return first_peer(mine(BACK_INNER, BACK_OUTER), i)

    def start_piece(copy, first, i):
        def start(s, carry):
            p = first(i) + lax.rem(lax.rem(me, eighth) + s, eighth)

            @pl.when(p != me)
            def _():
                copy(p, me).start()

            return carry

        lax.fori_loop(0, eighth, start, 0)

    def arrange(i):
        begin = pl.multiple_of(first_out(i) * per_peer, piece)
        place = begin + lax.broadcasted_iota(jnp.int32, (piece, LANES), 0)
        pick = jnp.concatenate([one_hot_bf16(place == p) for p in pos], axis=1)
        send[pl.ds(begin, piece), :] = joined(dot(pick, sorted_terms[...]), width)

    def start_ids(step, carry):
        ids_copy(lax.rem(me + step, n), me).start()
        return carry

    arrange(0)
    pl.semaphore_wait(barrier, n - 1)
    lax.fori_loop(1, n, start_ids, 0)
    start_piece(grads_copy, first_out, 0)
    arrange(1)

    @pl.loop(2, 8)
    def _(i):
        arrange(i)
        start_piece(grads_copy, first_out, i - 1)

    recv_ids[pl.ds(me, 1)] = send_ids[pl.ds(me, 1)]

    def ids_arrive(step, carry):
        p = lax.rem(me + step, n)
        ids_copy(p, p).wait_recv()
        return carry

    lax.fori_loop(1, n, ids_arrive, 0)
    start_piece(grads_copy, first_out, 7)
    rows_of(recv, me)[...] = rows_of(send, me)[...]
    for b in range(blocks):
        line = sum(recv_ids[b * per_row + k] for k in range(per_row))
        ids_ref[b : b + 1, :] = jnp.clip(line, 0, rows_dev - 1)
    to_smem = pltpu.make_async_copy(ids_ref, ids_smem, smem_sem)
    to_smem.start()

    @pl.loop(0, blocks)
    def _(b):
        here = pl.ds(pl.multiple_of(b * LANES, LANES), LANES)
        cols[here, :] = column_of(ids_ref[pl.ds(b, 1), :])

    loads[2].wait()
    acc3 = jnp.concatenate(split3(accum[...]), axis=1)
    terms[:, 3 * width : 4 * width] = jnp.ones((tile, width), BF16)

    to_smem.wait()
    loads[3].wait()

    @pl.loop(0, blocks)
    def _(b):
        start = pl.multiple_of(b * LANES, LANES)
        for i in range(0, LANES, BATCH):
            batch = [table[pl.ds(ids_smem[b, i + k], 1), :] for k in range(BATCH)]
            for k in range(BATCH):
                old_rows[pl.ds(start + i + k, 1), :] = batch[k]

    lines = piece // LANES
    other = 2 * side + 1 - lax.rem(floor, 2)
    near, far = quarter_at(1 - side, 1), quarter_at(1 - side, 0)

    def receive(pieces):
        rows = []
        for k, source in enumerate(pieces):

            def arrive(s, carry, source=source):
                p = source * eighth + s

                @pl.when(p != me)
                def _():
                    grads_copy(p, p).wait_recv()

                return carry

            lax.fori_loop(0, eighth, arrive, 0)
            begin = pl.multiple_of(source * piece, piece)
            fill(terms.at[k * piece : (k + 1) * piece, :], recv[pl.ds(begin, piece), :], width)
            rows += [ids_ref[pl.ds(source * lines + j, 1), :] for j in range(lines)]
        return rows

    def added(here, rows):
        col = cols[here, :]
        same = jnp.concatenate([one_hot_bf16(col == r) for r in rows], axis=1)
        return dot(same, terms[...])

    def pieces_at(i):
        group = digit_of(mine(IN_INNER, IN_OUTER), i)
        cross, odd = group // 2, lax.rem(group, 2)
        whole = floor * (1 - odd) + other * odd
        turn = row * (1 - odd) + (1 - row) * odd
        return [
            (1 - cross) * 2 * whole + cross * (2 * near + turn),
            (1 - cross) * (2 * whole + 1) + cross * (2 * far + turn),
        ]

    def add_source(i):
        rows = receive(pieces_at(i))

        @pl.loop(0, 4)
        def _(t):
            here = pl.ds(pl.multiple_of(t * tile, tile), tile)
            if isinstance(i, int):
                acc[here, :] = added(here, rows)
            else:
                acc[here, :] += added(here, rows)

    add_source(0)

    @pl.loop(1, 3)
    def _(i):
        add_source(i)

    last = receive(pieces_at(3))
    lane = lax.broadcasted_iota(jnp.int32, (piece, LANES), 1)
    group_iota = lax.broadcasted_iota(jnp.int32, (piece, groups), 1)

    @pl.loop(0, 8)
    def _(i):
        here = pl.ds(pl.multiple_of(first_back(i) * per_peer, piece), piece)
        col = cols[here, :]
        out = acc[here, :] + added(here, last)
        summed = joined(out, width)
        times = out[:, 3 * width : 3 * width + 1]
        mean = jnp.sum(summed * summed, axis=1, keepdims=True) * (1.0 / width)
        at_lane = (col & (LANES - 1)) == lane
        at_group = one_hot_bf16((col >> 7)[:, 0:1] == group_iota)
        found = joined(dot(at_group, acc3), LANES)
        new_acc = jnp.sum(jnp.where(at_lane, found, 0.0), axis=1, keepdims=True) + mean
        rate = LEARNING_RATE / (jnp.sqrt(new_acc) + EPSILON)
        fresh[here, :] = old_rows[here, :] - summed * rate
        share = jnp.where(at_lane, jnp.broadcast_to(mean / times, (piece, LANES)), 0.0)
        for k, term in enumerate(split3(share)):
            weights[here, k * LANES : (k + 1) * LANES] = term
        hi_hot[here, :] = at_group

        @pl.when(i > 0)
        def _():
            start_piece(back_copy, first_back, i - 1)

    means = lax.dot_general(
        hi_hot[...], weights[...], (((0,), (0,)), ((), ())), preferred_element_type=F32
    )
    new_accum_ref[...] = accum[...] + joined(means, LANES)
    start_piece(back_copy, first_back, 7)
    rows_of(back, me)[...] = rows_of(fresh, me)[...]

    def back_arrive(step, carry):
        p = lax.rem(me + step, n)
        back_copy(p, p).wait_recv()
        return carry

    lax.fori_loop(1, n, back_arrive, 0)

    def drain(step, carry):
        p = lax.rem(me + step, n)
        ids_copy(p, me).wait_send()
        grads_copy(p, me).wait_send()
        back_copy(p, me).wait_send()
        return carry

    lax.fori_loop(1, n, drain, 0)


def finish_kernel(
    pos_smem, ids_smem, fresh, back, accum, table_in,
    new_table, new_accum, looked_up, table,
    rows, table_sem, accum_sem, rows_sem,
):
    del table_in
    look = fresh.shape[0]
    blocks = look // LANES
    tile = look // 4
    keep = pltpu.make_async_copy(accum, new_accum, accum_sem)
    keep.start()

    @pl.loop(0, blocks)
    def _(b):
        start = pl.multiple_of(b * LANES, LANES)
        for i in range(0, LANES, BATCH):
            batch = [fresh[pl.ds(start + i + k, 1), :] for k in range(BATCH)]
            for k in range(BATCH):
                table[pl.ds(ids_smem[b, i + k], 1), :] = batch[k]

    store = pltpu.make_async_copy(table, new_table, table_sem)
    store.start()

    def out_copy(t):
        here = pl.ds(pl.multiple_of(t * tile, tile), tile)
        return pltpu.make_async_copy(rows.at[here, :], looked_up.at[here, :], rows_sem.at[t])

    @pl.loop(0, 4)
    def _(t):
        @pl.loop(0, tile // LANES)
        def _(j):
            b = t * (tile // LANES) + j
            start = pl.multiple_of(b * LANES, LANES)
            for i in range(0, LANES, BATCH):
                batch = [back[pl.ds(pos_smem[b, i + k], 1), :] for k in range(BATCH)]
                for k in range(BATCH):
                    rows[pl.ds(start + i + k, 1), :] = batch[k]

        @pl.when(t > 0)
        def _():
            out_copy(t - 1).start()

    keep.wait()
    out_copy(3).start()
    for t in range(4):
        out_copy(t).wait()
    store.wait()


def in_hbm(x):
    return pltpu.with_memory_space_constraint(x, pltpu.HBM)


def on_device(lookup_ids, grad_rows, emb_table, row_accum):
    n = lax.axis_size("shard")
    look, width = grad_rows.shape
    rows_dev = emb_table.shape[0]
    blocks = look // LANES
    groups = rows_dev // LANES
    vmem = pl.BlockSpec(memory_space=pltpu.VMEM)
    smem = pl.BlockSpec(memory_space=pltpu.SMEM)
    hbm = pl.BlockSpec(memory_space=pltpu.HBM)
    tile = look // 4
    dma = pltpu.SemaphoreType.DMA

    pos, local_ids, fresh, accum, table, back = pl.pallas_call(
        functools.partial(step_kernel, n),
        out_shape=[
            pltpu.VMEM((blocks, LANES), jnp.int32),
            pltpu.VMEM((blocks, LANES), jnp.int32),
            pltpu.VMEM((look, width), F32),
            pltpu.VMEM((groups, LANES), F32),
            pltpu.VMEM((rows_dev, width), F32),
            pltpu.VMEM((look, width), F32),
        ],
        in_specs=[hbm] * 4,
        out_specs=[vmem] * 6,
        scratch_shapes=[
            pltpu.VMEM((blocks, LANES), jnp.int32),
            pltpu.VMEM((look, width), F32),
            pltpu.VMEM((groups, LANES), F32),
            pltpu.VMEM((n, 1, LANES), jnp.int32),
            pltpu.VMEM((look, width), F32),
            pltpu.VMEM((n, 1, LANES), jnp.int32),
            pltpu.VMEM((look, width), F32),
            pltpu.VMEM((look, 3 * width), BF16),
            pltpu.VMEM((tile, 4 * width), BF16),
            pltpu.VMEM((look, 4 * width), F32),
            pltpu.VMEM((look, LANES), jnp.int32),
            pltpu.VMEM((look, width), F32),
            pltpu.VMEM((look, 3 * LANES), BF16),
            pltpu.VMEM((look, groups), BF16),
            pltpu.SMEM((blocks, LANES), jnp.int32),
            dma((4,)),
            dma(()),
            dma((n,)),
            dma((n,)),
            dma((n,)),
            dma((n,)),
            dma((n,)),
            dma((n,)),
        ],
        compiler_params=pltpu.CompilerParams(
            collective_id=1, has_side_effects=True, vmem_limit_bytes=44 * MIB
        ),
    )(
        in_hbm(lookup_ids.reshape(blocks, LANES)),
        in_hbm(grad_rows),
        in_hbm(row_accum.reshape(groups, LANES)),
        in_hbm(emb_table),
    )

    new_table, new_accum, looked_up, _ = pl.pallas_call(
        finish_kernel,
        out_shape=[
            jax.ShapeDtypeStruct((rows_dev, width), F32),
            jax.ShapeDtypeStruct((groups, LANES), F32),
            jax.ShapeDtypeStruct((look, width), F32),
            pltpu.VMEM((rows_dev, width), F32),
        ],
        in_specs=[smem, smem, vmem, vmem, vmem, vmem],
        out_specs=[hbm, hbm, hbm, vmem],
        input_output_aliases={5: 3},
        scratch_shapes=[pltpu.VMEM((look, width), F32), dma(()), dma(()), dma((4,))],
        compiler_params=pltpu.CompilerParams(vmem_limit_bytes=24 * MIB),
    )(pos, local_ids, fresh, back, accum, table)
    return (new_table, new_accum.reshape(rows_dev), looked_up)


def solution(mesh):
    in_specs = (P("shard"), P("shard", None), P("shard", None), P("shard"))
    out_specs = (P("shard", None), P("shard"), P("shard", None))
    return jax.shard_map(
        on_device, mesh=mesh, in_specs=in_specs, out_specs=out_specs, check_vma=False
    )
```

```python
import functools

import jax
import jax.numpy as jnp
from jax import lax
from jax.experimental import pallas as pl
from jax.experimental.pallas import tpu as pltpu
from jax.sharding import PartitionSpec as P

LEARNING_RATE = 0.5
EPSILON = 1e-08
LANES = 128
MIB = 1024 * 1024
BATCH = 16
MESH = pl.DeviceIdType.MESH


def order_of(*pieces):
    return sum(piece * 8**i for i, piece in enumerate(pieces))


OUT = order_of(6, 7, 0, 1, 2, 3, 4, 5)
IN_INNER = order_of(2, 3, 1, 0)
IN_OUTER = order_of(0, 1, 2, 3)
BACK_INNER = order_of(4, 6, 0, 5, 7, 1, 2, 3)
BACK_OUTER = order_of(2, 3, 4, 6, 5, 7, 0, 1)
F32 = jnp.float32
BF16 = jnp.bfloat16


def split3(x):
    hi = x.astype(BF16)
    rest = x - hi.astype(F32)
    mid = rest.astype(BF16)
    low = (rest - mid.astype(F32)).astype(BF16)
    return hi, mid, low


def dot(a, b):
    return jnp.dot(a, b, preferred_element_type=F32)


def column_of(row):
    return jnp.transpose(jnp.broadcast_to(row, (LANES, LANES)))


def one_hot_bf16(mask):
    return jnp.where(mask, 1.0, 0.0).astype(BF16)


def fill(terms, x, width):
    for i, term in enumerate(split3(x)):
        terms[:, i * width : (i + 1) * width] = term


def joined(x, width):
    return x[:, 0:width] + x[:, width : 2 * width] + x[:, 2 * width : 3 * width]


def quarter_at(half, inner):
    return inner * (1 + half) + (1 - inner) * 3 * half


def greet_all(barrier, me, n):
    def greet(step, carry):
        pl.semaphore_signal(
            barrier, inc=1, device_id=(lax.rem(me + step, n),), device_id_type=MESH
        )
        return carry

    lax.fori_loop(1, n, greet, 0)


def step_kernel(
    n, ids_hbm, grads_hbm, accum_hbm, emb_hbm,
    pos_ref, ids_ref, fresh, new_accum_ref, table, back,
    lookups, grads, accum, send_ids, send, recv_ids, recv, sorted_terms, terms, acc, cols, old_rows,
    weights, hi_hot, ids_smem,
    load_sem, smem_sem, ids_out, ids_in, grads_out, grads_in, back_out, back_in,
):
    blocks = lookups.shape[0]
    look = blocks * LANES
    width = grads.shape[1]
    rows_dev = table.shape[0]
    groups = accum.shape[0]
    per_peer = look // n
    per_row = LANES // per_peer
    quarter = n // 4
    eighth = n // 8
    piece = look // 8
    tile = look // 4
    me = lax.axis_index("shard")
    side = me // (n // 2)
    floor = me // quarter
    inner = lax.rem(floor + side, 2)
    row = lax.rem(me, quarter) // eighth
    loads = [
        pltpu.make_async_copy(s, d, load_sem.at[i])
        for i, (s, d) in enumerate(
            ((ids_hbm, lookups), (grads_hbm, grads), (accum_hbm, accum), (emb_hbm, table))
        )
    ]
    barrier = pltpu.get_barrier_semaphore()
    for load in loads:
        load.start()
    greet_all(barrier, me, n)

    loads[0].wait()
    peer_iota = lax.broadcasted_iota(jnp.int32, (n, LANES), 0)
    slot_iota = lax.broadcasted_iota(jnp.int32, (LANES, LANES), 0)
    before = one_hot_bf16(slot_iota < lax.broadcasted_iota(jnp.int32, (LANES, LANES), 1))
    shift = lax.rem(me, per_row) * per_peer
    base = jnp.zeros((n, 1), F32)
    low = peer_iota * rows_dev
    owned, ranked, pos = [], [], []
    for b in range(blocks):
        ids = lookups[b : b + 1, :]
        mine = (ids >= low) & (ids < low + rows_dev)
        hot = jnp.where(mine, 1.0, 0.0)
        rank = dot(hot.astype(BF16), before) + base
        rank = jnp.sum(hot * rank, axis=0, keepdims=True).astype(jnp.int32)
        peer = jnp.sum(jnp.where(mine, peer_iota, 0), axis=0, keepdims=True)
        pos.append(peer * per_peer + rank)
        pos_ref[b : b + 1, :] = pos[b]
        base = base + jnp.sum(hot, axis=1, keepdims=True)
        offset = ids - peer * rows_dev
        digits = [offset & 255, (offset >> 8) & 255, offset >> 16]
        owned.append(jnp.concatenate([hot * d.astype(F32) for d in digits], axis=0).astype(BF16))
        ranked.append(one_hot_bf16(slot_iota == rank + shift))
    named = lax.dot_general(
        jnp.concatenate(owned, axis=1),
        jnp.concatenate(ranked, axis=1),
        (((1,), (1,)), ((), ())),
        preferred_element_type=F32,
    ).astype(jnp.int32)
    named = named[0:n] + named[n : 2 * n] * 256 + named[2 * n : 3 * n] * 65536
    for p in range(n):
        send_ids[p] = named[p : p + 1, :]
    loads[1].wait()
    fill(sorted_terms, grads[...], width)

    def rows_of(ref, p):
        return ref.at[pl.ds(pl.multiple_of(p * per_peer, 8), per_peer), :]

    def ids_copy(p, source):
        return pltpu.make_async_remote_copy(
            src_ref=send_ids.at[p], dst_ref=recv_ids.at[source],
            send_sem=ids_out, recv_sem=ids_in,
            device_id=(p,), device_id_type=MESH,
        )

    def grads_copy(p, source):
        return pltpu.make_async_remote_copy(
            src_ref=rows_of(send, p), dst_ref=rows_of(recv, source),
            send_sem=grads_out, recv_sem=grads_in.at[source // eighth],
            device_id=(p,), device_id_type=MESH,
        )

    def back_copy(p, source):
        return pltpu.make_async_remote_copy(
            src_ref=rows_of(fresh, p), dst_ref=rows_of(back, source),
            send_sem=back_out, recv_sem=back_in,
            device_id=(p,), device_id_type=MESH,
        )

    def wait_rows(ref, begin, rows, sem):
        here = ref.at[pl.ds(begin, rows), :]
        pltpu.make_async_copy(here, here, sem).wait()

    def mine(at_inner, at_outer):
        return inner * at_inner + (1 - inner) * at_outer

    def digit_of(order, i):
        return lax.rem(lax.shift_right_logical(jnp.int32(order), jnp.int32(3 * i)), 8)

    def first_peer(order, i):
        piece_at = digit_of(order, i)
        cross, middle, turn = piece_at // 4, lax.rem(piece_at // 2, 2), lax.rem(piece_at, 2)
        half = cross * (1 - side) + (1 - cross) * side
        return quarter_at(half, middle) * quarter + lax.rem(row + turn, 2) * eighth

    def first_out(i):
        return first_peer(OUT, i)

    def first_back(i):
        return first_peer(mine(BACK_INNER, BACK_OUTER), i)

    def start_piece(copy, first, i):
        def start(s, carry):
            p = first(i) + lax.rem(lax.rem(me, eighth) + s, eighth)

            @pl.when(p != me)
            def _():
                copy(p, me).start()

            return carry

        lax.fori_loop(0, eighth, start, 0)

    def arrange(i):
        begin = pl.multiple_of(first_out(i) * per_peer, piece)
        place = begin + lax.broadcasted_iota(jnp.int32, (piece, LANES), 0)
        pick = jnp.concatenate([one_hot_bf16(place == p) for p in pos], axis=1)
        send[pl.ds(begin, piece), :] = joined(dot(pick, sorted_terms[...]), width)

    def start_ids(step, carry):
        ids_copy(lax.rem(me + step, n), me).start()
        return carry

    arrange(0)
    pl.semaphore_wait(barrier, n - 1)
    lax.fori_loop(1, n, start_ids, 0)
    start_piece(grads_copy, first_out, 0)
    arrange(1)

    @pl.loop(2, 8)
    def _(i):
        arrange(i)
        start_piece(grads_copy, first_out, i - 1)

    recv_ids[pl.ds(me, 1)] = send_ids[pl.ds(me, 1)]

    others = recv_ids.at[pl.ds(0, n - 1)]
    pltpu.make_async_copy(others, others, ids_in).wait()
    start_piece(grads_copy, first_out, 7)
    rows_of(recv, me)[...] = rows_of(send, me)[...]
    for b in range(blocks):
        line = sum(recv_ids[b * per_row + k] for k in range(per_row))
        ids_ref[b : b + 1, :] = jnp.clip(line, 0, rows_dev - 1)
    to_smem = pltpu.make_async_copy(ids_ref, ids_smem, smem_sem)
    to_smem.start()

    @pl.loop(0, blocks)
    def _(b):
        here = pl.ds(pl.multiple_of(b * LANES, LANES), LANES)
        cols[here, :] = column_of(ids_ref[pl.ds(b, 1), :])

    loads[2].wait()
    acc3 = jnp.concatenate(split3(accum[...]), axis=1)
    terms[:, 3 * width : 4 * width] = jnp.ones((tile, width), BF16)

    to_smem.wait()
    loads[3].wait()

    @pl.loop(0, blocks)
    def _(b):
        start = pl.multiple_of(b * LANES, LANES)
        for i in range(0, LANES, BATCH):
            batch = [table[pl.ds(ids_smem[b, i + k], 1), :] for k in range(BATCH)]
            for k in range(BATCH):
                old_rows[pl.ds(start + i + k, 1), :] = batch[k]

    lines = piece // LANES
    other = 2 * side + 1 - lax.rem(floor, 2)
    near, far = quarter_at(1 - side, 1), quarter_at(1 - side, 0)

    def receive(pieces):
        rows = []
        for k, source in enumerate(pieces):

            begin = pl.multiple_of(source * piece, piece)

            @pl.when(source == me // eighth)
            def _(begin=begin, source=source):
                wait_rows(recv, begin, piece - per_peer, grads_in.at[source])

            @pl.when(source != me // eighth)
            def _(begin=begin, source=source):
                wait_rows(recv, begin, piece, grads_in.at[source])

            fill(terms.at[k * piece : (k + 1) * piece, :], recv[pl.ds(begin, piece), :], width)
            rows += [ids_ref[pl.ds(source * lines + j, 1), :] for j in range(lines)]
        return rows

    def added(here, rows):
        col = cols[here, :]
        same = jnp.concatenate([one_hot_bf16(col == r) for r in rows], axis=1)
        return dot(same, terms[...])

    def pieces_at(i):
        group = digit_of(mine(IN_INNER, IN_OUTER), i)
        cross, odd = group // 2, lax.rem(group, 2)
        whole = floor * (1 - odd) + other * odd
        turn = row * (1 - odd) + (1 - row) * odd
        return [
            (1 - cross) * 2 * whole + cross * (2 * near + turn),
            (1 - cross) * (2 * whole + 1) + cross * (2 * far + turn),
        ]

    def add_source(i):
        rows = receive(pieces_at(i))

        @pl.loop(0, 4)
        def _(t):
            here = pl.ds(pl.multiple_of(t * tile, tile), tile)
            if isinstance(i, int):
                acc[here, :] = added(here, rows)
            else:
                acc[here, :] += added(here, rows)

    add_source(0)

    @pl.loop(1, 3)
    def _(i):
        add_source(i)

    last = receive(pieces_at(3))
    lane = lax.broadcasted_iota(jnp.int32, (piece, LANES), 1)
    group_iota = lax.broadcasted_iota(jnp.int32, (piece, groups), 1)

    @pl.loop(0, 8)
    def _(i):
        here = pl.ds(pl.multiple_of(first_back(i) * per_peer, piece), piece)
        col = cols[here, :]
        out = acc[here, :] + added(here, last)
        summed = joined(out, width)
        times = out[:, 3 * width : 3 * width + 1]
        mean = jnp.sum(summed * summed, axis=1, keepdims=True) * (1.0 / width)
        at_lane = (col & (LANES - 1)) == lane
        at_group = one_hot_bf16((col >> 7)[:, 0:1] == group_iota)
        found = joined(dot(at_group, acc3), LANES)
        new_acc = jnp.sum(jnp.where(at_lane, found, 0.0), axis=1, keepdims=True) + mean
        rate = LEARNING_RATE / (jnp.sqrt(new_acc) + EPSILON)
        fresh[here, :] = old_rows[here, :] - summed * rate
        share = jnp.where(at_lane, jnp.broadcast_to(mean / times, (piece, LANES)), 0.0)
        for k, term in enumerate(split3(share)):
            weights[here, k * LANES : (k + 1) * LANES] = term
        hi_hot[here, :] = at_group

        @pl.when(i > 0)
        def _():
            start_piece(back_copy, first_back, i - 1)

    means = lax.dot_general(
        hi_hot[...], weights[...], (((0,), (0,)), ((), ())), preferred_element_type=F32
    )
    new_accum_ref[...] = accum[...] + joined(means, LANES)
    start_piece(back_copy, first_back, 7)
    rows_of(back, me)[...] = rows_of(fresh, me)[...]

    wait_rows(back, 0, look - per_peer, back_in)
    pltpu.make_async_copy(others, others, ids_out).wait()
    wait_rows(send, 0, look - per_peer, grads_out)
    wait_rows(fresh, 0, look - per_peer, back_out)


def finish_kernel(
    pos_smem, ids_smem, fresh, back, accum, table_in,
    new_table, new_accum, looked_up, table,
    rows, table_sem, accum_sem, rows_sem,
):
    del table_in
    look = fresh.shape[0]
    blocks = look // LANES
    tile = look // 4
    keep = pltpu.make_async_copy(accum, new_accum, accum_sem)
    keep.start()

    @pl.loop(0, blocks)
    def _(b):
        start = pl.multiple_of(b * LANES, LANES)
        for i in range(0, LANES, BATCH):
            batch = [fresh[pl.ds(start + i + k, 1), :] for k in range(BATCH)]
            for k in range(BATCH):
                table[pl.ds(ids_smem[b, i + k], 1), :] = batch[k]

    store = pltpu.make_async_copy(table, new_table, table_sem)
    store.start()

    def out_copy(t):
        here = pl.ds(pl.multiple_of(t * tile, tile), tile)
        return pltpu.make_async_copy(rows.at[here, :], looked_up.at[here, :], rows_sem.at[t])

    @pl.loop(0, 4)
    def _(t):
        @pl.loop(0, tile // LANES)
        def _(j):
            b = t * (tile // LANES) + j
            start = pl.multiple_of(b * LANES, LANES)
            for i in range(0, LANES, BATCH):
                batch = [back[pl.ds(pos_smem[b, i + k], 1), :] for k in range(BATCH)]
                for k in range(BATCH):
                    rows[pl.ds(start + i + k, 1), :] = batch[k]

        @pl.when(t > 0)
        def _():
            out_copy(t - 1).start()

    keep.wait()
    out_copy(3).start()
    for t in range(4):
        out_copy(t).wait()
    store.wait()


def in_hbm(x):
    return pltpu.with_memory_space_constraint(x, pltpu.HBM)


def on_device(lookup_ids, grad_rows, emb_table, row_accum):
    n = lax.axis_size("shard")
    look, width = grad_rows.shape
    rows_dev = emb_table.shape[0]
    blocks = look // LANES
    groups = rows_dev // LANES
    vmem = pl.BlockSpec(memory_space=pltpu.VMEM)
    smem = pl.BlockSpec(memory_space=pltpu.SMEM)
    hbm = pl.BlockSpec(memory_space=pltpu.HBM)
    tile = look // 4
    dma = pltpu.SemaphoreType.DMA

    pos, local_ids, fresh, accum, table, back = pl.pallas_call(
        functools.partial(step_kernel, n),
        out_shape=[
            pltpu.VMEM((blocks, LANES), jnp.int32),
            pltpu.VMEM((blocks, LANES), jnp.int32),
            pltpu.VMEM((look, width), F32),
            pltpu.VMEM((groups, LANES), F32),
            pltpu.VMEM((rows_dev, width), F32),
            pltpu.VMEM((look, width), F32),
        ],
        in_specs=[hbm] * 4,
        out_specs=[vmem] * 6,
        scratch_shapes=[
            pltpu.VMEM((blocks, LANES), jnp.int32),
            pltpu.VMEM((look, width), F32),
            pltpu.VMEM((groups, LANES), F32),
            pltpu.VMEM((n, 1, LANES), jnp.int32),
            pltpu.VMEM((look, width), F32),
            pltpu.VMEM((n, 1, LANES), jnp.int32),
            pltpu.VMEM((look, width), F32),
            pltpu.VMEM((look, 3 * width), BF16),
            pltpu.VMEM((tile, 4 * width), BF16),
            pltpu.VMEM((look, 4 * width), F32),
            pltpu.VMEM((look, LANES), jnp.int32),
            pltpu.VMEM((look, width), F32),
            pltpu.VMEM((look, 3 * LANES), BF16),
            pltpu.VMEM((look, groups), BF16),
            pltpu.SMEM((blocks, LANES), jnp.int32),
            dma((4,)),
            dma(()),
            dma(()),
            dma(()),
            dma(()),
            dma((8,)),
            dma(()),
            dma(()),
        ],
        compiler_params=pltpu.CompilerParams(
            collective_id=1, has_side_effects=True, vmem_limit_bytes=44 * MIB
        ),
    )(
        in_hbm(lookup_ids.reshape(blocks, LANES)),
        in_hbm(grad_rows),
        in_hbm(row_accum.reshape(groups, LANES)),
        in_hbm(emb_table),
    )

    new_table, new_accum, looked_up, _ = pl.pallas_call(
        finish_kernel,
        out_shape=[
            jax.ShapeDtypeStruct((rows_dev, width), F32),
            jax.ShapeDtypeStruct((groups, LANES), F32),
            jax.ShapeDtypeStruct((look, width), F32),
            pltpu.VMEM((rows_dev, width), F32),
        ],
        in_specs=[smem, smem, vmem, vmem, vmem, vmem],
        out_specs=[hbm, hbm, hbm, vmem],
        input_output_aliases={5: 3},
        scratch_shapes=[pltpu.VMEM((look, width), F32), dma(()), dma(()), dma((4,))],
        compiler_params=pltpu.CompilerParams(vmem_limit_bytes=24 * MIB),
    )(pos, local_ids, fresh, back, accum, table)
    return (new_table, new_accum.reshape(rows_dev), looked_up)


def solution(mesh):
    in_specs = (P("shard"), P("shard", None), P("shard", None), P("shard"))
    out_specs = (P("shard", None), P("shard"), P("shard", None))
    return jax.shard_map(
        on_device, mesh=mesh, in_specs=in_specs, out_specs=out_specs, check_vma=False
    )
```

```python
import functools

import jax
import jax.numpy as jnp
from jax import lax
from jax.experimental import pallas as pl
from jax.experimental.pallas import tpu as pltpu
from jax.sharding import PartitionSpec as P

LEARNING_RATE = 0.5
EPSILON = 1e-08
LANES = 128
MIB = 1024 * 1024
BATCH = 16
SEGMENTS = 8
MESH = pl.DeviceIdType.MESH


def order_of(*pieces):
    return sum(piece * 8**i for i, piece in enumerate(pieces))


OUT = order_of(6, 7, 0, 1, 2, 3, 4, 5)
IN_INNER = order_of(2, 3, 1, 0)
IN_OUTER = order_of(0, 1, 2, 3)
BACK_INNER = order_of(4, 6, 0, 5, 7, 1, 2, 3)
BACK_OUTER = order_of(2, 3, 4, 6, 5, 7, 0, 1)
F32 = jnp.float32
BF16 = jnp.bfloat16


def split3(x):
    hi = x.astype(BF16)
    rest = x - hi.astype(F32)
    mid = rest.astype(BF16)
    low = (rest - mid.astype(F32)).astype(BF16)
    return hi, mid, low


def dot(a, b):
    return jnp.dot(a, b, preferred_element_type=F32)


def column_of(row):
    return jnp.transpose(jnp.broadcast_to(row, (LANES, LANES)))


def one_hot_bf16(mask):
    return jnp.where(mask, 1.0, 0.0).astype(BF16)


def fill(terms, x, width):
    for i, term in enumerate(split3(x)):
        terms[:, i * width : (i + 1) * width] = term


def joined(x, width):
    return x[:, 0:width] + x[:, width : 2 * width] + x[:, 2 * width : 3 * width]


def quarter_at(half, inner):
    return inner * (1 + half) + (1 - inner) * 3 * half


def greet_all(barrier, me, n):
    def greet(step, carry):
        pl.semaphore_signal(
            barrier, inc=1, device_id=(lax.rem(me + step, n),), device_id_type=MESH
        )
        return carry

    lax.fori_loop(1, n, greet, 0)


def step_kernel(
    n, ids_hbm, grads_hbm, accum_hbm, emb_hbm,
    plan, fresh, new_accum_ref, table, back,
    ids_ref, lookups, grads, accum, send_ids, send, recv_ids, recv, sorted_terms, terms, acc, cols, old_rows,
    weights, hi_hot, prior, ids_smem,
    load_sem, smem_sem, ids_out, ids_in, grads_out, grads_in, back_out, back_in,
):
    blocks = lookups.shape[0]
    look = blocks * LANES
    width = grads.shape[1]
    rows_dev = table.shape[0]
    groups = accum.shape[0]
    per_peer = look // n
    per_row = LANES // per_peer
    quarter = n // 4
    eighth = n // 8
    low_rows = rows_dev // SEGMENTS
    piece = look // 8
    tile = look // 4
    me = lax.axis_index("shard")
    side = me // (n // 2)
    floor = me // quarter
    inner = lax.rem(floor + side, 2)
    row = lax.rem(me, quarter) // eighth
    loads = [
        pltpu.make_async_copy(s, d, load_sem.at[i])
        for i, (s, d) in enumerate(
            ((ids_hbm, lookups), (grads_hbm, grads), (accum_hbm, accum), (emb_hbm, table))
        )
    ]
    barrier = pltpu.get_barrier_semaphore()
    for load in loads[:2]:
        load.start()
    greet_all(barrier, me, n)
    for load in loads[2:]:
        load.start()

    loads[0].wait()
    peer_iota = lax.broadcasted_iota(jnp.int32, (n, LANES), 0)
    slot_iota = lax.broadcasted_iota(jnp.int32, (LANES, LANES), 0)
    before = one_hot_bf16(slot_iota < lax.broadcasted_iota(jnp.int32, (LANES, LANES), 1))
    shift = lax.rem(me, per_row) * per_peer
    base = jnp.zeros((n, 1), F32)
    low = peer_iota * rows_dev
    owned, ranked, pos = [], [], []
    for b in range(blocks):
        ids = lookups[b : b + 1, :]
        mine = (ids >= low) & (ids < low + rows_dev)
        hot = jnp.where(mine, 1.0, 0.0)
        rank = dot(hot.astype(BF16), before) + base
        rank = jnp.sum(hot * rank, axis=0, keepdims=True).astype(jnp.int32)
        peer = jnp.sum(jnp.where(mine, peer_iota, 0), axis=0, keepdims=True)
        pos.append(peer * per_peer + rank)
        plan[b : b + 1, :] = pos[b]
        base = base + jnp.sum(hot, axis=1, keepdims=True)
        offset = ids - peer * rows_dev
        digits = [offset & 255, (offset >> 8) & 255, offset >> 16]
        owned.append(jnp.concatenate([hot * d.astype(F32) for d in digits], axis=0).astype(BF16))
        ranked.append(one_hot_bf16(slot_iota == rank + shift))
    named = lax.dot_general(
        jnp.concatenate(owned, axis=1),
        jnp.concatenate(ranked, axis=1),
        (((1,), (1,)), ((), ())),
        preferred_element_type=F32,
    ).astype(jnp.int32)
    named = named[0:n] + named[n : 2 * n] * 256 + named[2 * n : 3 * n] * 65536
    for p in range(n):
        send_ids[p] = named[p : p + 1, :]
    loads[1].wait()
    fill(sorted_terms, grads[...], width)

    def rows_of(ref, p):
        return ref.at[pl.ds(pl.multiple_of(p * per_peer, 8), per_peer), :]

    def ids_copy(p, source):
        return pltpu.make_async_remote_copy(
            src_ref=send_ids.at[p], dst_ref=recv_ids.at[source],
            send_sem=ids_out, recv_sem=ids_in,
            device_id=(p,), device_id_type=MESH,
        )

    def grads_copy(p, source):
        return pltpu.make_async_remote_copy(
            src_ref=rows_of(send, p), dst_ref=rows_of(recv, source),
            send_sem=grads_out, recv_sem=grads_in.at[source // eighth],
            device_id=(p,), device_id_type=MESH,
        )

    def back_copy(p, source):
        return pltpu.make_async_remote_copy(
            src_ref=rows_of(fresh, p), dst_ref=rows_of(back, source),
            send_sem=back_out, recv_sem=back_in,
            device_id=(p,), device_id_type=MESH,
        )

    def wait_rows(ref, begin, rows, sem):
        here = ref.at[pl.ds(begin, rows), :]
        pltpu.make_async_copy(here, here, sem).wait()

    def mine(at_inner, at_outer):
        return inner * at_inner + (1 - inner) * at_outer

    def digit_of(order, i):
        return lax.rem(lax.shift_right_logical(jnp.int32(order), jnp.int32(3 * i)), 8)

    def first_peer(order, i):
        piece_at = digit_of(order, i)
        cross, middle, turn = piece_at // 4, lax.rem(piece_at // 2, 2), lax.rem(piece_at, 2)
        half = cross * (1 - side) + (1 - cross) * side
        return quarter_at(half, middle) * quarter + lax.rem(row + turn, 2) * eighth

    def first_out(i):
        return first_peer(OUT, i)

    def first_back(i):
        return first_peer(mine(BACK_INNER, BACK_OUTER), i)

    def start_piece(copy, first, i):
        def start(s, carry):
            p = first(i) + lax.rem(lax.rem(me, eighth) + s, eighth)

            @pl.when(p != me)
            def _():
                copy(p, me).start()

            return carry

        lax.fori_loop(0, eighth, start, 0)

    def arrange(i):
        begin = pl.multiple_of(first_out(i) * per_peer, piece)
        place = begin + lax.broadcasted_iota(jnp.int32, (piece, LANES), 0)
        pick = jnp.concatenate([one_hot_bf16(place == p) for p in pos], axis=1)
        send[pl.ds(begin, piece), :] = joined(dot(pick, sorted_terms[...]), width)

    def start_ids(step, carry):
        ids_copy(lax.rem(me + step, n), me).start()
        return carry

    arrange(0)
    pl.semaphore_wait(barrier, n - 1)
    lax.fori_loop(1, n, start_ids, 0)
    start_piece(grads_copy, first_out, 0)
    arrange(1)

    @pl.loop(2, 8)
    def _(i):
        arrange(i)
        start_piece(grads_copy, first_out, i - 1)

    recv_ids[pl.ds(me, 1)] = send_ids[pl.ds(me, 1)]

    others = recv_ids.at[pl.ds(0, n - 1)]
    pltpu.make_async_copy(others, others, ids_in).wait()
    start_piece(grads_copy, first_out, 7)
    rows_of(recv, me)[...] = rows_of(send, me)[...]
    for b in range(blocks):
        line = sum(recv_ids[b * per_row + k] for k in range(per_row))
        ids_ref[b : b + 1, :] = jnp.clip(line, 0, rows_dev - 1)
    to_smem = pltpu.make_async_copy(ids_ref, ids_smem, smem_sem)
    to_smem.start()

    @pl.loop(0, blocks)
    def _(b):
        here = pl.ds(pl.multiple_of(b * LANES, LANES), LANES)
        cols[here, :] = column_of(ids_ref[pl.ds(b, 1), :])

    loads[2].wait()
    acc3 = jnp.concatenate(split3(accum[...]), axis=1)
    terms[:, 3 * width : 4 * width] = jnp.ones((tile, width), BF16)

    to_smem.wait()
    loads[3].wait()

    @pl.loop(0, blocks)
    def _(b):
        start = pl.multiple_of(b * LANES, LANES)
        for i in range(0, LANES, BATCH):
            batch = [table[pl.ds(ids_smem[b, i + k], 1), :] for k in range(BATCH)]
            for k in range(BATCH):
                old_rows[pl.ds(start + i + k, 1), :] = batch[k]

    lane = lax.broadcasted_iota(jnp.int32, (piece, LANES), 1)
    group_iota = lax.broadcasted_iota(jnp.int32, (piece, groups), 1)

    @pl.loop(0, 8)
    def _(i):
        here = pl.ds(pl.multiple_of(i * piece, piece), piece)
        col = cols[here, :]
        at_lane = (col & (LANES - 1)) == lane
        at_group = one_hot_bf16((col >> 7)[:, 0:1] == group_iota)
        hi_hot[here, :] = at_group
        found = joined(dot(at_group, acc3), LANES)
        prior[here, :] = jnp.sum(jnp.where(at_lane, found, 0.0), axis=1, keepdims=True)

    lines = piece // LANES
    other = 2 * side + 1 - lax.rem(floor, 2)
    near, far = quarter_at(1 - side, 1), quarter_at(1 - side, 0)

    def receive(pieces):
        rows = []
        for k, source in enumerate(pieces):

            begin = pl.multiple_of(source * piece, piece)

            @pl.when(source == me // eighth)
            def _(begin=begin, source=source):
                wait_rows(recv, begin, piece - per_peer, grads_in.at[source])

            @pl.when(source != me // eighth)
            def _(begin=begin, source=source):
                wait_rows(recv, begin, piece, grads_in.at[source])

            fill(terms.at[k * piece : (k + 1) * piece, :], recv[pl.ds(begin, piece), :], width)
            rows += [ids_ref[pl.ds(source * lines + j, 1), :] for j in range(lines)]
        return rows

    def added(here, rows):
        col = cols[here, :]
        same = jnp.concatenate([one_hot_bf16(col == r) for r in rows], axis=1)
        return dot(same, terms[...])

    def pieces_at(i):
        group = digit_of(mine(IN_INNER, IN_OUTER), i)
        cross, odd = group // 2, lax.rem(group, 2)
        whole = floor * (1 - odd) + other * odd
        turn = row * (1 - odd) + (1 - row) * odd
        return [
            (1 - cross) * 2 * whole + cross * (2 * near + turn),
            (1 - cross) * (2 * whole + 1) + cross * (2 * far + turn),
        ]

    def add_source(i):
        rows = receive(pieces_at(i))

        @pl.loop(0, 4)
        def _(t):
            here = pl.ds(pl.multiple_of(t * tile, tile), tile)
            if isinstance(i, int):
                acc[here, :] = added(here, rows)
            else:
                acc[here, :] += added(here, rows)

    add_source(0)

    @pl.loop(1, 3)
    def _(i):
        add_source(i)

    last = receive(pieces_at(3))
    @pl.loop(0, 8)
    def _(i):
        here = pl.ds(pl.multiple_of(first_back(i) * per_peer, piece), piece)
        out = acc[here, :] + added(here, last)
        acc[here, :] = out
        summed = joined(out, width)
        mean = jnp.sum(summed * summed, axis=1, keepdims=True) * (1.0 / width)
        rate = LEARNING_RATE / (jnp.sqrt(prior[here, :] + mean) + EPSILON)
        step = summed * rate
        fresh[here, :] = old_rows[here, :] - step
        old_rows[here, :] = step

        @pl.when(i > 0)
        def _():
            start_piece(back_copy, first_back, i - 1)

    rows_of(back, me)[...] = rows_of(fresh, me)[...]

    @pl.loop(0, 8)
    def _(i):
        here = pl.ds(pl.multiple_of(i * piece, piece), piece)

        @pl.when(i == 1)
        def _():
            start_piece(back_copy, first_back, 7)

        out = acc[here, :]
        summed = joined(out, width)
        mean = jnp.sum(summed * summed, axis=1, keepdims=True) * (1.0 / width)
        part = 1.0 / out[:, 3 * width : 3 * width + 1]
        fill(sorted_terms.at[here, :], old_rows[here, :] * part, width)
        at_lane = (cols[here, :] & (LANES - 1)) == lane
        share = jnp.where(at_lane, jnp.broadcast_to(mean * part, (piece, LANES)), 0.0)
        for k, term in enumerate(split3(share)):
            weights[here, k * LANES : (k + 1) * LANES] = term

    means = lax.dot_general(
        hi_hot[...], weights[...], (((0,), (0,)), ((), ())), preferred_element_type=F32
    )
    new_accum_ref[...] = accum[...] + joined(means, LANES)

    base = jnp.zeros((1, 1), F32)
    line_iota = lax.broadcasted_iota(jnp.int32, (blocks, LANES), 0)
    lane_row = lax.broadcasted_iota(jnp.int32, (1, LANES), 1)
    owned, ranked = [], []
    for b in range(blocks):
        line = ids_ref[b : b + 1, :]
        high = jnp.where(line >= low_rows, 1.0, 0.0)
        place = jnp.where(line >= low_rows, dot(high.astype(BF16), before) + base, -1.0)
        place = place.astype(jnp.int32)
        base = base + jnp.sum(high, axis=1, keepdims=True)
        hot = jnp.where(line_iota == place >> 7, 1.0, 0.0)
        digits = [line & 255, (line >> 8) & 255, line >> 16, lane_row, jnp.full_like(line, b)]
        digits.append(jnp.ones_like(line))
        owned.append(jnp.concatenate([hot * d.astype(F32) for d in digits], axis=0).astype(BF16))
        ranked.append(one_hot_bf16((slot_iota == place & (LANES - 1)) & (place >= 0)))
    listed = lax.dot_general(
        jnp.concatenate(owned, axis=1),
        jnp.concatenate(ranked, axis=1),
        (((1,), (1,)), ((), ())),
        preferred_element_type=F32,
    ).astype(jnp.int32)
    named = [listed[i * blocks : (i + 1) * blocks] for i in range(6)]
    high_rows = named[0] + named[1] * 256 + named[2] * 65536
    both = high_rows * look + named[3] + named[4] * LANES
    both = jnp.where(named[5] > 0, both, jnp.broadcast_to(both[0:1, 0:1], (blocks, LANES)))
    total = jnp.broadcast_to(base.astype(jnp.int32), (8, LANES))
    plan[blocks :, :] = jnp.concatenate([total[0:1], both, total[1:]], axis=0)
    rows = [ids_ref[b : b + 1, :] for b in range(blocks)]

    @pl.loop(0, low_rows // piece)
    def _(i):
        begin = pl.multiple_of(i * piece, piece)
        here = pl.ds(begin, piece)
        place = begin + lax.broadcasted_iota(jnp.int32, (piece, LANES), 0)
        pick = jnp.concatenate([one_hot_bf16(place == r) for r in rows], axis=1)
        table[here, :] -= joined(dot(pick, sorted_terms[...]), width)

    wait_rows(back, 0, look - per_peer, back_in)
    pltpu.make_async_copy(others, others, ids_out).wait()
    wait_rows(send, 0, look - per_peer, grads_out)
    wait_rows(fresh, 0, look - per_peer, back_out)


def finish_kernel(
    plan_ref, fresh, back, accum, table_in,
    new_table, new_accum, looked_up, table,
    rows, plan, plan_sem, table_sem, accum_sem, rows_sem,
):
    del table_in
    look = fresh.shape[0]
    blocks = look // LANES
    tile = look // 4
    segment = table.shape[0] // SEGMENTS
    def read(part, begin, count):
        here = pl.ds(begin, count)
        return pltpu.make_async_copy(plan_ref.at[here, :], plan.at[here, :], plan_sem.at[part])

    head, tail, order = read(0, blocks, 8), read(1, blocks + 8, blocks), read(2, 0, blocks)
    head.start()
    keep = pltpu.make_async_copy(accum, new_accum, accum_sem)
    keep.start()

    def store(i):
        here = pl.ds(pl.multiple_of(i * segment, segment), segment)
        return pltpu.make_async_copy(table.at[here, :], new_table.at[here, :], table_sem.at[i])

    store(0).start()
    head.wait()
    order.start()
    lines = (plan[blocks, 0] + LANES - 1) // LANES

    shift = look.bit_length() - 1

    def scatter(begin, end):
        @pl.loop(begin, end)
        def _(b):
            for i in range(0, LANES, BATCH):
                both = [plan[blocks + 1 + b, i + k] for k in range(BATCH)]
                batch = [fresh[pl.ds(v & (look - 1), 1), :] for v in both]
                for v, values in zip(both, batch):
                    table[pl.ds(v >> shift, 1), :] = values

    scatter(0, jnp.minimum(lines, 7))

    @pl.when(lines > 7)
    def _():
        tail.start()
        tail.wait()
        scatter(7, lines)

    for i in range(1, SEGMENTS):
        store(i).start()
    order.wait()

    def out_copy(t):
        here = pl.ds(pl.multiple_of(t * tile, tile), tile)
        return pltpu.make_async_copy(rows.at[here, :], looked_up.at[here, :], rows_sem.at[t])

    @pl.loop(0, 4)
    def _(t):
        @pl.loop(0, tile // LANES)
        def _(j):
            b = t * (tile // LANES) + j
            start = pl.multiple_of(b * LANES, LANES)
            for i in range(0, LANES, BATCH):
                batch = [back[pl.ds(plan[b, i + k], 1), :] for k in range(BATCH)]
                for k in range(BATCH):
                    rows[pl.ds(start + i + k, 1), :] = batch[k]

        @pl.when(t > 0)
        def _():
            out_copy(t - 1).start()

    keep.wait()
    out_copy(3).start()
    for t in range(4):
        out_copy(t).wait()
    for i in range(SEGMENTS):
        store(i).wait()


def in_hbm(x):
    return pltpu.with_memory_space_constraint(x, pltpu.HBM)


def on_device(lookup_ids, grad_rows, emb_table, row_accum):
    n = lax.axis_size("shard")
    look, width = grad_rows.shape
    rows_dev = emb_table.shape[0]
    blocks = look // LANES
    groups = rows_dev // LANES
    vmem = pl.BlockSpec(memory_space=pltpu.VMEM)
    hbm = pl.BlockSpec(memory_space=pltpu.HBM)
    tile = look // 4
    dma = pltpu.SemaphoreType.DMA

    plan, fresh, accum, table, back = pl.pallas_call(
        functools.partial(step_kernel, n),
        out_shape=[
            pltpu.VMEM((2 * blocks + 8, LANES), jnp.int32),
            pltpu.VMEM((look, width), F32),
            pltpu.VMEM((groups, LANES), F32),
            pltpu.VMEM((rows_dev, width), F32),
            pltpu.VMEM((look, width), F32),
        ],
        in_specs=[hbm] * 4,
        out_specs=[vmem] * 5,
        scratch_shapes=[
            pltpu.VMEM((blocks, LANES), jnp.int32),
            pltpu.VMEM((blocks, LANES), jnp.int32),
            pltpu.VMEM((look, width), F32),
            pltpu.VMEM((groups, LANES), F32),
            pltpu.VMEM((n, 1, LANES), jnp.int32),
            pltpu.VMEM((look, width), F32),
            pltpu.VMEM((n, 1, LANES), jnp.int32),
            pltpu.VMEM((look, width), F32),
            pltpu.VMEM((look, 3 * width), BF16),
            pltpu.VMEM((tile, 4 * width), BF16),
            pltpu.VMEM((look, 4 * width), F32),
            pltpu.VMEM((look, LANES), jnp.int32),
            pltpu.VMEM((look, width), F32),
            pltpu.VMEM((look, 3 * LANES), BF16),
            pltpu.VMEM((look, groups), BF16),
            pltpu.VMEM((look, 1), F32),
            pltpu.SMEM((blocks, LANES), jnp.int32),
            dma((4,)),
            dma(()),
            dma(()),
            dma(()),
            dma(()),
            dma((8,)),
            dma(()),
            dma(()),
        ],
        compiler_params=pltpu.CompilerParams(
            collective_id=1, has_side_effects=True, vmem_limit_bytes=44 * MIB
        ),
    )(
        in_hbm(lookup_ids.reshape(blocks, LANES)),
        in_hbm(grad_rows),
        in_hbm(row_accum.reshape(groups, LANES)),
        in_hbm(emb_table),
    )

    new_table, new_accum, looked_up, _ = pl.pallas_call(
        finish_kernel,
        out_shape=[
            jax.ShapeDtypeStruct((rows_dev, width), F32),
            jax.ShapeDtypeStruct((groups, LANES), F32),
            jax.ShapeDtypeStruct((look, width), F32),
            pltpu.VMEM((rows_dev, width), F32),
        ],
        in_specs=[vmem] * 5,
        out_specs=[hbm, hbm, hbm, vmem],
        input_output_aliases={4: 3},
        scratch_shapes=[
            pltpu.VMEM((look, width), F32),
            pltpu.SMEM((2 * blocks + 8, LANES), jnp.int32),
            dma((3,)),
            dma((SEGMENTS,)),
            dma(()),
            dma((4,)),
        ],
        compiler_params=pltpu.CompilerParams(vmem_limit_bytes=24 * MIB),
    )(plan, fresh, back, accum, table)
    return (new_table, new_accum.reshape(rows_dev), looked_up)


def solution(mesh):
    in_specs = (P("shard"), P("shard", None), P("shard", None), P("shard"))
    out_specs = (P("shard", None), P("shard"), P("shard", None))
    return jax.shard_map(
        on_device, mesh=mesh, in_specs=in_specs, out_specs=out_specs, check_vma=False
    )
```

```python
import functools

import jax
import jax.numpy as jnp
from jax import lax
from jax.experimental import pallas as pl
from jax.experimental.pallas import tpu as pltpu
from jax.sharding import PartitionSpec as P

LEARNING_RATE = 0.5
EPSILON = 1e-08
LANES = 128
MIB = 1024 * 1024
BATCH = 16
SEGMENTS = 8
MESH = pl.DeviceIdType.MESH


def order_of(*pieces):
    return sum(piece * 8**i for i, piece in enumerate(pieces))


OUT = order_of(6, 7, 0, 1, 2, 3, 4, 5)
IN_INNER = order_of(2, 3, 1, 0)
IN_OUTER = order_of(0, 1, 2, 3)
BACK_INNER = order_of(4, 6, 0, 5, 7, 1, 2, 3)
BACK_OUTER = order_of(2, 3, 4, 5, 6, 7, 0, 1)
F32 = jnp.float32
BF16 = jnp.bfloat16


def split3(x):
    hi = x.astype(BF16)
    rest = x - hi.astype(F32)
    mid = rest.astype(BF16)
    low = (rest - mid.astype(F32)).astype(BF16)
    return hi, mid, low


def dot(a, b):
    return jnp.dot(a, b, preferred_element_type=F32)


def column_of(row):
    return jnp.transpose(jnp.broadcast_to(row, (LANES, LANES)))


def one_hot_bf16(mask):
    return jnp.where(mask, 1.0, 0.0).astype(BF16)


def fill(terms, x, width):
    for i, term in enumerate(split3(x)):
        terms[:, i * width : (i + 1) * width] = term


def joined(x, width):
    return x[:, 0:width] + x[:, width : 2 * width] + x[:, 2 * width : 3 * width]


def quarter_at(half, inner):
    return inner * (1 + half) + (1 - inner) * 3 * half


def greet_all(barrier, me, n):
    def greet(step, carry):
        pl.semaphore_signal(
            barrier, inc=1, device_id=(lax.rem(me + step, n),), device_id_type=MESH
        )
        return carry

    lax.fori_loop(1, n, greet, 0)


def step_kernel(
    n, ids_hbm, grads_hbm, accum_hbm, emb_hbm,
    plan, fresh, new_accum_ref, table, back,
    ids_ref, lookups, grads, accum, send_ids, send, recv_ids, recv, sorted_terms, terms, acc, cols, old_rows,
    weights, hi_hot, prior, ids_smem,
    load_sem, smem_sem, ids_out, ids_in, grads_out, grads_in, back_out, back_in,
):
    blocks = lookups.shape[0]
    look = blocks * LANES
    width = grads.shape[1]
    rows_dev = table.shape[0]
    groups = accum.shape[0]
    per_peer = look // n
    per_row = LANES // per_peer
    quarter = n // 4
    eighth = n // 8
    piece = look // 8
    tile = look // 4
    me = lax.axis_index("shard")
    side = me // (n // 2)
    floor = me // quarter
    inner = lax.rem(floor + side, 2)
    row = lax.rem(me, quarter) // eighth
    low_rows = (1 + 2 * inner) * (rows_dev // SEGMENTS)
    loads = [
        pltpu.make_async_copy(s, d, load_sem.at[i])
        for i, (s, d) in enumerate(
            ((ids_hbm, lookups), (grads_hbm, grads), (accum_hbm, accum), (emb_hbm, table))
        )
    ]
    barrier = pltpu.get_barrier_semaphore()
    for load in loads[:2]:
        load.start()
    greet_all(barrier, me, n)
    for load in loads[2:]:
        load.start()

    loads[0].wait()
    peer_iota = lax.broadcasted_iota(jnp.int32, (n, LANES), 0)
    slot_iota = lax.broadcasted_iota(jnp.int32, (LANES, LANES), 0)
    before = one_hot_bf16(slot_iota < lax.broadcasted_iota(jnp.int32, (LANES, LANES), 1))
    shift = lax.rem(me, per_row) * per_peer
    base = jnp.zeros((n, 1), F32)
    low = peer_iota * rows_dev
    owned, ranked, pos = [], [], []
    for b in range(blocks):
        ids = lookups[b : b + 1, :]
        mine = (ids >= low) & (ids < low + rows_dev)
        hot = jnp.where(mine, 1.0, 0.0)
        rank = dot(hot.astype(BF16), before) + base
        rank = jnp.sum(hot * rank, axis=0, keepdims=True).astype(jnp.int32)
        peer = jnp.sum(jnp.where(mine, peer_iota, 0), axis=0, keepdims=True)
        pos.append(peer * per_peer + rank)
        plan[b : b + 1, :] = pos[b]
        base = base + jnp.sum(hot, axis=1, keepdims=True)
        offset = ids - peer * rows_dev
        digits = [offset & 255, (offset >> 8) & 255, offset >> 16]
        owned.append(jnp.concatenate([hot * d.astype(F32) for d in digits], axis=0).astype(BF16))
        ranked.append(one_hot_bf16(slot_iota == rank + shift))
    named = lax.dot_general(
        jnp.concatenate(owned, axis=1),
        jnp.concatenate(ranked, axis=1),
        (((1,), (1,)), ((), ())),
        preferred_element_type=F32,
    ).astype(jnp.int32)
    named = named[0:n] + named[n : 2 * n] * 256 + named[2 * n : 3 * n] * 65536
    for p in range(n):
        send_ids[p] = named[p : p + 1, :]
    loads[1].wait()
    fill(sorted_terms, grads[...], width)

    def rows_of(ref, p):
        return ref.at[pl.ds(pl.multiple_of(p * per_peer, 8), per_peer), :]

    def ids_copy(p, source):
        return pltpu.make_async_remote_copy(
            src_ref=send_ids.at[p], dst_ref=recv_ids.at[source],
            send_sem=ids_out, recv_sem=ids_in,
            device_id=(p,), device_id_type=MESH,
        )

    def grads_copy(p, source):
        return pltpu.make_async_remote_copy(
            src_ref=rows_of(send, p), dst_ref=rows_of(recv, source),
            send_sem=grads_out, recv_sem=grads_in.at[source // eighth],
            device_id=(p,), device_id_type=MESH,
        )

    def back_copy(p, source):
        return pltpu.make_async_remote_copy(
            src_ref=rows_of(fresh, p), dst_ref=rows_of(back, source),
            send_sem=back_out, recv_sem=back_in,
            device_id=(p,), device_id_type=MESH,
        )

    def wait_rows(ref, begin, rows, sem):
        here = ref.at[pl.ds(begin, rows), :]
        pltpu.make_async_copy(here, here, sem).wait()

    def mine(at_inner, at_outer):
        return inner * at_inner + (1 - inner) * at_outer

    def digit_of(order, i):
        return lax.rem(lax.shift_right_logical(jnp.int32(order), jnp.int32(3 * i)), 8)

    def first_peer(order, i):
        piece_at = digit_of(order, i)
        cross, middle, turn = piece_at // 4, lax.rem(piece_at // 2, 2), lax.rem(piece_at, 2)
        half = cross * (1 - side) + (1 - cross) * side
        return quarter_at(half, middle) * quarter + lax.rem(row + turn, 2) * eighth

    def first_out(i):
        return first_peer(OUT, i)

    def first_back(i):
        return first_peer(mine(BACK_INNER, BACK_OUTER), i)

    def start_piece(copy, first, i):
        def start(s, carry):
            p = first(i) + lax.rem(lax.rem(me, eighth) + s, eighth)

            @pl.when(p != me)
            def _():
                copy(p, me).start()

            return carry

        lax.fori_loop(0, eighth, start, 0)

    def arrange(i):
        begin = pl.multiple_of(first_out(i) * per_peer, piece)
        place = begin + lax.broadcasted_iota(jnp.int32, (piece, LANES), 0)
        pick = jnp.concatenate([one_hot_bf16(place == p) for p in pos], axis=1)
        send[pl.ds(begin, piece), :] = joined(dot(pick, sorted_terms[...]), width)

    def start_ids(step, carry):
        ids_copy(lax.rem(me + step, n), me).start()
        return carry

    arrange(0)
    pl.semaphore_wait(barrier, n - 1)
    lax.fori_loop(1, n, start_ids, 0)
    start_piece(grads_copy, first_out, 0)
    arrange(1)

    @pl.loop(2, 8)
    def _(i):
        arrange(i)
        start_piece(grads_copy, first_out, i - 1)

    recv_ids[pl.ds(me, 1)] = send_ids[pl.ds(me, 1)]

    others = recv_ids.at[pl.ds(0, n - 1)]
    pltpu.make_async_copy(others, others, ids_in).wait()
    start_piece(grads_copy, first_out, 7)
    rows_of(recv, me)[...] = rows_of(send, me)[...]
    for b in range(blocks):
        line = sum(recv_ids[b * per_row + k] for k in range(per_row))
        ids_ref[b : b + 1, :] = jnp.clip(line, 0, rows_dev - 1)
    to_smem = pltpu.make_async_copy(ids_ref, ids_smem, smem_sem)
    to_smem.start()

    @pl.loop(0, blocks)
    def _(b):
        here = pl.ds(pl.multiple_of(b * LANES, LANES), LANES)
        cols[here, :] = column_of(ids_ref[pl.ds(b, 1), :])

    loads[2].wait()
    acc3 = jnp.concatenate(split3(accum[...]), axis=1)
    terms[:, 3 * width : 4 * width] = jnp.ones((tile, width), BF16)

    to_smem.wait()
    loads[3].wait()

    @pl.loop(0, blocks)
    def _(b):
        start = pl.multiple_of(b * LANES, LANES)
        for i in range(0, LANES, BATCH):
            batch = [table[pl.ds(ids_smem[b, i + k], 1), :] for k in range(BATCH)]
            for k in range(BATCH):
                old_rows[pl.ds(start + i + k, 1), :] = batch[k]

    lane = lax.broadcasted_iota(jnp.int32, (piece, LANES), 1)
    group_iota = lax.broadcasted_iota(jnp.int32, (piece, groups), 1)

    @pl.loop(0, 8)
    def _(i):
        here = pl.ds(pl.multiple_of(i * piece, piece), piece)
        col = cols[here, :]
        at_lane = (col & (LANES - 1)) == lane
        at_group = one_hot_bf16((col >> 7)[:, 0:1] == group_iota)
        hi_hot[here, :] = at_group
        found = joined(dot(at_group, acc3), LANES)
        prior[here, :] = jnp.sum(jnp.where(at_lane, found, 0.0), axis=1, keepdims=True)

    lines = piece // LANES
    other = 2 * side + 1 - lax.rem(floor, 2)
    near, far = quarter_at(1 - side, 1), quarter_at(1 - side, 0)

    def receive(pieces):
        rows = []
        for k, source in enumerate(pieces):

            begin = pl.multiple_of(source * piece, piece)

            @pl.when(source == me // eighth)
            def _(begin=begin, source=source):
                wait_rows(recv, begin, piece - per_peer, grads_in.at[source])

            @pl.when(source != me // eighth)
            def _(begin=begin, source=source):
                wait_rows(recv, begin, piece, grads_in.at[source])

            fill(terms.at[k * piece : (k + 1) * piece, :], recv[pl.ds(begin, piece), :], width)
            rows += [ids_ref[pl.ds(source * lines + j, 1), :] for j in range(lines)]
        return rows

    def added(here, rows):
        col = cols[here, :]
        same = jnp.concatenate([one_hot_bf16(col == r) for r in rows], axis=1)
        return dot(same, terms[...])

    def pieces_at(i):
        group = digit_of(mine(IN_INNER, IN_OUTER), i)
        cross, odd = group // 2, lax.rem(group, 2)
        whole = floor * (1 - odd) + other * odd
        turn = row * (1 - odd) + (1 - row) * odd
        return [
            (1 - cross) * 2 * whole + cross * (2 * near + turn),
            (1 - cross) * (2 * whole + 1) + cross * (2 * far + turn),
        ]

    def add_source(i):
        rows = receive(pieces_at(i))

        @pl.loop(0, 4)
        def _(t):
            here = pl.ds(pl.multiple_of(t * tile, tile), tile)
            if isinstance(i, int):
                acc[here, :] = added(here, rows)
            else:
                acc[here, :] += added(here, rows)

    add_source(0)

    @pl.loop(1, 3)
    def _(i):
        add_source(i)

    last = receive(pieces_at(3))
    @pl.loop(0, 8)
    def _(i):
        here = pl.ds(pl.multiple_of(first_back(i) * per_peer, piece), piece)
        out = acc[here, :] + added(here, last)
        acc[here, :] = out
        summed = joined(out, width)
        mean = jnp.sum(summed * summed, axis=1, keepdims=True) * (1.0 / width)
        rate = LEARNING_RATE / (jnp.sqrt(prior[here, :] + mean) + EPSILON)
        step = summed * rate
        fresh[here, :] = old_rows[here, :] - step
        old_rows[here, :] = step

        @pl.when(i > 0)
        def _():
            start_piece(back_copy, first_back, i - 1)

    rows_of(back, me)[...] = rows_of(fresh, me)[...]

    @pl.loop(0, 8)
    def _(i):
        here = pl.ds(pl.multiple_of(i * piece, piece), piece)

        @pl.when(i == 1)
        def _():
            start_piece(back_copy, first_back, 7)

        out = acc[here, :]
        summed = joined(out, width)
        mean = jnp.sum(summed * summed, axis=1, keepdims=True) * (1.0 / width)
        part = 1.0 / out[:, 3 * width : 3 * width + 1]
        fill(sorted_terms.at[here, :], old_rows[here, :] * part, width)
        at_lane = (cols[here, :] & (LANES - 1)) == lane
        share = jnp.where(at_lane, jnp.broadcast_to(mean * part, (piece, LANES)), 0.0)
        for k, term in enumerate(split3(share)):
            weights[here, k * LANES : (k + 1) * LANES] = term

    means = lax.dot_general(
        hi_hot[...], weights[...], (((0,), (0,)), ((), ())), preferred_element_type=F32
    )
    new_accum_ref[...] = accum[...] + joined(means, LANES)

    base = jnp.zeros((1, 1), F32)
    line_iota = lax.broadcasted_iota(jnp.int32, (blocks, LANES), 0)
    lane_row = lax.broadcasted_iota(jnp.int32, (1, LANES), 1)
    owned, ranked = [], []
    for b in range(blocks):
        line = ids_ref[b : b + 1, :]
        high = jnp.where(line >= low_rows, 1.0, 0.0)
        place = jnp.where(line >= low_rows, dot(high.astype(BF16), before) + base, -1.0)
        place = place.astype(jnp.int32)
        base = base + jnp.sum(high, axis=1, keepdims=True)
        hot = jnp.where(line_iota == place >> 7, 1.0, 0.0)
        digits = [line & 255, (line >> 8) & 255, line >> 16, lane_row, jnp.full_like(line, b)]
        digits.append(jnp.ones_like(line))
        owned.append(jnp.concatenate([hot * d.astype(F32) for d in digits], axis=0).astype(BF16))
        ranked.append(one_hot_bf16((slot_iota == place & (LANES - 1)) & (place >= 0)))
    listed = lax.dot_general(
        jnp.concatenate(owned, axis=1),
        jnp.concatenate(ranked, axis=1),
        (((1,), (1,)), ((), ())),
        preferred_element_type=F32,
    ).astype(jnp.int32)
    named = [listed[i * blocks : (i + 1) * blocks] for i in range(6)]
    high_rows = named[0] + named[1] * 256 + named[2] * 65536
    both = high_rows * look + named[3] + named[4] * LANES
    both = jnp.where(named[5] > 0, both, jnp.broadcast_to(both[0:1, 0:1], (blocks, LANES)))
    total = jnp.broadcast_to(base.astype(jnp.int32), (8, LANES))
    plan[blocks :, :] = jnp.concatenate([total[0:1], both, total[1:]], axis=0)
    rows = [ids_ref[b : b + 1, :] for b in range(blocks)]

    @pl.loop(0, low_rows // piece)
    def _(i):
        begin = pl.multiple_of(i * piece, piece)
        here = pl.ds(begin, piece)
        place = begin + lax.broadcasted_iota(jnp.int32, (piece, LANES), 0)
        pick = jnp.concatenate([one_hot_bf16(place == r) for r in rows], axis=1)
        table[here, :] -= joined(dot(pick, sorted_terms[...]), width)

    wait_rows(back, 0, look - per_peer, back_in)
    pltpu.make_async_copy(others, others, ids_out).wait()
    wait_rows(send, 0, look - per_peer, grads_out)
    wait_rows(fresh, 0, look - per_peer, back_out)


def finish_kernel(
    plan_ref, fresh, back, accum, table_in,
    new_table, new_accum, looked_up, table,
    rows, plan, plan_sem, table_sem, accum_sem, rows_sem,
):
    del table_in
    look = fresh.shape[0]
    blocks = look // LANES
    tile = look // 4
    segment = table.shape[0] // SEGMENTS
    def read(part, begin, count):
        here = pl.ds(begin, count)
        return pltpu.make_async_copy(plan_ref.at[here, :], plan.at[here, :], plan_sem.at[part])

    head, tail, order = read(0, blocks, 8), read(1, blocks + 8, blocks), read(2, 0, blocks)
    head.start()
    keep = pltpu.make_async_copy(accum, new_accum, accum_sem)
    keep.start()

    def store(i):
        here = pl.ds(pl.multiple_of(i * segment, segment), segment)
        return pltpu.make_async_copy(table.at[here, :], new_table.at[here, :], table_sem.at[i])

    store(0).start()
    head.wait()
    order.start()
    lines = (plan[blocks, 0] + LANES - 1) // LANES

    shift = look.bit_length() - 1

    def scatter(begin, end):
        @pl.loop(begin, end)
        def _(b):
            for i in range(0, LANES, BATCH):
                both = [plan[blocks + 1 + b, i + k] for k in range(BATCH)]
                batch = [fresh[pl.ds(v & (look - 1), 1), :] for v in both]
                for v, values in zip(both, batch):
                    table[pl.ds(v >> shift, 1), :] = values

    scatter(0, jnp.minimum(lines, 7))

    @pl.when(lines > 7)
    def _():
        tail.start()
        tail.wait()
        scatter(7, lines)

    for i in range(1, SEGMENTS):
        store(i).start()
    order.wait()

    def out_copy(t):
        here = pl.ds(pl.multiple_of(t * tile, tile), tile)
        return pltpu.make_async_copy(rows.at[here, :], looked_up.at[here, :], rows_sem.at[t])

    @pl.loop(0, 4)
    def _(t):
        @pl.loop(0, tile // LANES)
        def _(j):
            b = t * (tile // LANES) + j
            start = pl.multiple_of(b * LANES, LANES)
            for i in range(0, LANES, BATCH):
                batch = [back[pl.ds(plan[b, i + k], 1), :] for k in range(BATCH)]
                for k in range(BATCH):
                    rows[pl.ds(start + i + k, 1), :] = batch[k]

        @pl.when(t > 0)
        def _():
            out_copy(t - 1).start()

    keep.wait()
    out_copy(3).start()
    for t in range(4):
        out_copy(t).wait()
    for i in range(SEGMENTS):
        store(i).wait()


def in_hbm(x):
    return pltpu.with_memory_space_constraint(x, pltpu.HBM)


def on_device(lookup_ids, grad_rows, emb_table, row_accum):
    n = lax.axis_size("shard")
    look, width = grad_rows.shape
    rows_dev = emb_table.shape[0]
    blocks = look // LANES
    groups = rows_dev // LANES
    vmem = pl.BlockSpec(memory_space=pltpu.VMEM)
    hbm = pl.BlockSpec(memory_space=pltpu.HBM)
    tile = look // 4
    dma = pltpu.SemaphoreType.DMA

    plan, fresh, accum, table, back = pl.pallas_call(
        functools.partial(step_kernel, n),
        out_shape=[
            pltpu.VMEM((2 * blocks + 8, LANES), jnp.int32),
            pltpu.VMEM((look, width), F32),
            pltpu.VMEM((groups, LANES), F32),
            pltpu.VMEM((rows_dev, width), F32),
            pltpu.VMEM((look, width), F32),
        ],
        in_specs=[hbm] * 4,
        out_specs=[vmem] * 5,
        scratch_shapes=[
            pltpu.VMEM((blocks, LANES), jnp.int32),
            pltpu.VMEM((blocks, LANES), jnp.int32),
            pltpu.VMEM((look, width), F32),
            pltpu.VMEM((groups, LANES), F32),
            pltpu.VMEM((n, 1, LANES), jnp.int32),
            pltpu.VMEM((look, width), F32),
            pltpu.VMEM((n, 1, LANES), jnp.int32),
            pltpu.VMEM((look, width), F32),
            pltpu.VMEM((look, 3 * width), BF16),
            pltpu.VMEM((tile, 4 * width), BF16),
            pltpu.VMEM((look, 4 * width), F32),
            pltpu.VMEM((look, LANES), jnp.int32),
            pltpu.VMEM((look, width), F32),
            pltpu.VMEM((look, 3 * LANES), BF16),
            pltpu.VMEM((look, groups), BF16),
            pltpu.VMEM((look, 1), F32),
            pltpu.SMEM((blocks, LANES), jnp.int32),
            dma((4,)),
            dma(()),
            dma(()),
            dma(()),
            dma(()),
            dma((8,)),
            dma(()),
            dma(()),
        ],
        compiler_params=pltpu.CompilerParams(
            collective_id=1, has_side_effects=True, vmem_limit_bytes=44 * MIB
        ),
    )(
        in_hbm(lookup_ids.reshape(blocks, LANES)),
        in_hbm(grad_rows),
        in_hbm(row_accum.reshape(groups, LANES)),
        in_hbm(emb_table),
    )

    new_table, new_accum, looked_up, _ = pl.pallas_call(
        finish_kernel,
        out_shape=[
            jax.ShapeDtypeStruct((rows_dev, width), F32),
            jax.ShapeDtypeStruct((groups, LANES), F32),
            jax.ShapeDtypeStruct((look, width), F32),
            pltpu.VMEM((rows_dev, width), F32),
        ],
        in_specs=[vmem] * 5,
        out_specs=[hbm, hbm, hbm, vmem],
        input_output_aliases={4: 3},
        scratch_shapes=[
            pltpu.VMEM((look, width), F32),
            pltpu.SMEM((2 * blocks + 8, LANES), jnp.int32),
            dma((3,)),
            dma((SEGMENTS,)),
            dma(()),
            dma((4,)),
        ],
        compiler_params=pltpu.CompilerParams(vmem_limit_bytes=24 * MIB),
    )(plan, fresh, back, accum, table)
    return (new_table, new_accum.reshape(rows_dev), looked_up)


def solution(mesh):
    in_specs = (P("shard"), P("shard", None), P("shard", None), P("shard"))
    out_specs = (P("shard", None), P("shard"), P("shard", None))
    return jax.shard_map(
        on_device, mesh=mesh, in_specs=in_specs, out_specs=out_specs, check_vma=False
    )
```
